512 devices in a mesh: gx: 4 (over y_hi), gy: 16 (over z, y_lo), gz: 8 (over x, core).
Axes of the slice: x: 4, y: 8 (y_hi: 4, y_lo: 2; y = y_hi * 2 + y_lo), z: 8, core: 2. Of those that a mesh axis runs over, the one named last changes fastest.
Arguments:
- nodal_scalar_values: float32 [3, 32, 128, 16384], P(None, 'gx', 'gy', 'gz'), may hold values from -6 to 6
- geometry: float32 [6, 4, 16, 2048], P(None, 'gx', 'gy', 'gz'), may hold values from -1.2 to 4, as said below
Outputs:
- assembled: float32 [3, 32, 128, 16384], P(None, 'gx', 'gy', 'gz')
The draws below stay inside these ranges and needn't reach their ends.
Inputs may be any that keep to these rules, and one draw needn't show every extreme that they name: `geometry`: G00, G11 and G22 are positive; each off-diagonal factor is at most 0.3 times the root of the product of its two diagonal factors in magnitude.
All inputs are finite; a program needn't handle non-finite values.
Results may differ from the reference program's by a relative error of at most 0.00007.
Values sent between devices are 32-bit elements; how exact they have to be, the bound alone decides.
A program may use at most 64 MiB of HBM per device.

```python
import math
import jax
import jax.numpy as jnp
import numpy as np
from jax import lax

COMPONENTS = 3
ELEMENTS_FIRST = 4
ELEMENTS_SECOND = 16
ELEMENTS_THIRD = 2048


def draw_geometry(key, part):
    element_grid_shape = (ELEMENTS_FIRST, ELEMENTS_SECOND, ELEMENTS_THIRD)
    key_list = jax.random.split(key, 2)
    diagonal = jnp.exp(jax.random.uniform(key_list[0], (3,) + element_grid_shape, jnp.float32, math.log(0.5), math.log(2.0)))
    coupling = jax.random.uniform(key_list[1], (3,) + element_grid_shape, jnp.float32, -0.3, 0.3)
    cross_xy = coupling[0] * jnp.sqrt(diagonal[0] * diagonal[1])
    cross_xz = coupling[1] * jnp.sqrt(diagonal[0] * diagonal[2])
    cross_yz = coupling[2] * jnp.sqrt(diagonal[1] * diagonal[2])
    return jnp.stack([diagonal[0], diagonal[1], diagonal[2], cross_xy, cross_xz, cross_yz]).astype(jnp.float32)


def level_of(own_key, extent, cuts, low, high):
    factor_of, own = 1.0, jax.random.fold_in(own_key, 6)
    for axis_at, blocks in cuts:
        steps = jnp.exp(jax.random.uniform(jax.random.fold_in(own, axis_at), (blocks,), jnp.float32, low / len(cuts), high / len(cuts)))
        factor_of = factor_of * jnp.repeat(steps, extent[axis_at] // blocks).reshape([-1 if axis == axis_at else 1 for axis in range(len(extent))])
    return factor_of


def gaussian(key, shape, scale, most, pieces=(), held_as=jnp.bfloat16):
    level = level_of(key, shape, pieces, -0.22, 0.18) if pieces else 1.0
    entries = jax.random.normal(key, shape, jnp.float32) * scale * level
    return jnp.minimum(jnp.maximum(entries, -most), most).astype(held_as)


def setup_inputs(seed: int = 0) -> dict:
    key_of = jax.random.split(jax.random.key(seed), 3)
    return {
        "nodal_scalar_values": gaussian(key_of[0], (COMPONENTS, 8 * ELEMENTS_FIRST, 8 * ELEMENTS_SECOND, 8 * ELEMENTS_THIRD), 1.0, 6.0, ((1, 4), (2, 16), (3, 8)), jnp.float32),
        "geometry": draw_geometry(jax.random.fold_in(key_of[2], 71), 0),
    }


interior_points = [-0.8717401485096066, -0.5917001814331423, -0.2092992179024789, 0.2092992179024789, 0.5917001814331423, 0.8717401485096066]


def legendre_seven(point):
    previous = 1.0
    current = point
    for order in range(1, 7):
        following = ((2 * order + 1) * point * current - order * previous) / (order + 1)
        previous = current
        current = following
    return current


def gll_tables():
    degree = 7
    points = [-1.0] + interior_points + [1.0]
    values = [legendre_seven(point) for point in points]
    node_count = degree + 1
    weights = np.array([2.0 / (degree * (degree + 1) * value * value) for value in values])
    derivative = np.zeros((node_count, node_count))
    for row_index in range(node_count):
        for col_index in range(node_count):
            if row_index != col_index:
                derivative[row_index, col_index] = values[row_index] / (values[col_index] * (points[row_index] - points[col_index]))
    derivative[0, 0] = -degree * (degree + 1) / 4.0
    derivative[node_count - 1, node_count - 1] = degree * (degree + 1) / 4.0
    return derivative, weights


def apply_axis(field_in, matrix, direction):
    length = field_in.shape[direction]
    block_size = math.gcd(length, 128)
    big_table = jnp.kron(jnp.eye(block_size // 8, dtype=jnp.float32), matrix)
    dim_list = list(field_in.shape)
    folded_shape = dim_list[:direction] + [length // block_size, block_size] + dim_list[direction + 1:]
    folded_field = field_in.reshape(folded_shape)
    patterns = ["nbyz,ab->nayz", "xnbz,ab->xnaz", "xynb,ab->xyna"]
    result = jnp.einsum(patterns[direction], folded_field, big_table, precision=lax.Precision.HIGHEST)
    return result.reshape(field_in.shape)


def expand(field_component, target):
    elem_x, elem_y, elem_z = field_component.shape
    spread = jnp.broadcast_to(field_component[:, None, :, None, :, None], (elem_x, 8, elem_y, 8, elem_z, 8))
    return spread.reshape(target)


def stiffness(field_in, geometry):
    derivative, weights = gll_tables()
    matrix = jnp.asarray(derivative, jnp.float32)
    weight_row = jnp.asarray(weights, jnp.float32)
    size_x, size_y, size_z = field_in.shape
    weight_x = jnp.tile(weight_row, size_x // 8)
    weight_y = jnp.tile(weight_row, size_y // 8)
    weight_z = jnp.tile(weight_row, size_z // 8)
    node_weight = weight_x[:, None, None] * weight_y[None, :, None] * weight_z[None, None, :]
    grad_x = apply_axis(field_in, matrix, 0)
    grad_y = apply_axis(field_in, matrix, 1)
    grad_z = apply_axis(field_in, matrix, 2)
    factors = [expand(geometry[index], field_in.shape) for index in range(6)]
    flux_x = node_weight * (factors[0] * grad_x + factors[3] * grad_y + factors[4] * grad_z)
    flux_y = node_weight * (factors[3] * grad_x + factors[1] * grad_y + factors[5] * grad_z)
    flux_z = node_weight * (factors[4] * grad_x + factors[5] * grad_y + factors[2] * grad_z)
    transposed = matrix.T
    return apply_axis(flux_x, transposed, 0) + apply_axis(flux_y, transposed, 1) + apply_axis(flux_z, transposed, 2)


def combine(middle, below_plane, above_plane, direction):
    length = middle.shape[direction]
    from_above = jnp.concatenate([lax.slice_in_dim(middle, 1, length, axis=direction), above_plane], axis=direction)
    from_below = jnp.concatenate([below_plane, lax.slice_in_dim(middle, 0, length - 1, axis=direction)], axis=direction)
    position = lax.broadcasted_iota(jnp.int32, middle.shape, direction) % 8
    return middle + jnp.where(position == 7, from_above, 0.0) + jnp.where(position == 0, from_below, 0.0)


def single_component(field_values, geometry):
    total_x, total_y, total_z = field_values.shape
    zblock = math.gcd(total_z, 1024)
    block_count = total_z // zblock
    field_blocks = jnp.moveaxis(field_values.reshape(total_x, total_y, block_count, zblock), 2, 0)
    geometries = jnp.moveaxis(geometry.reshape(6, geometry.shape[1], geometry.shape[2], block_count, zblock // 8), 3, 0)
    local_terms = lax.map(lambda operands: stiffness(operands[0], operands[1]), (field_blocks, geometries))
    local_terms = jnp.moveaxis(local_terms, 0, 2).reshape(field_values.shape)
    summed = local_terms
    for direction in range(3):
        plane_extents = list(summed.shape)
        plane_extents[direction] = 1
        zero_plane = jnp.zeros(plane_extents, jnp.float32)
        summed = combine(summed, zero_plane, zero_plane, direction)
    return summed


def reference(nodal_scalar_values, geometry):
    return jnp.stack([single_component(nodal_scalar_values[component], geometry) for component in range(COMPONENTS)])
```

```python
import functools

import jax
import jax.numpy as jnp
import numpy as np
from jax import lax
from jax.experimental import pallas as pl
from jax.experimental.pallas import tpu as pltpu
from jax.sharding import PartitionSpec as P

MESH = pl.DeviceIdType.MESH
F32 = jnp.float32
BF16 = jnp.bfloat16
LANES = 128

interior_points = [
    -0.8717401485096066,
    -0.5917001814331423,
    -0.2092992179024789,
    0.2092992179024789,
    0.5917001814331423,
    0.8717401485096066,
]


def legendre_seven(point):
    previous = 1.0
    current = point
    for order in range(1, 7):
        following = ((2 * order + 1) * point * current - order * previous) / (order + 1)
        previous = current
        current = following
    return current


def gll_tables():
    degree = 7
    points = [-1.0] + interior_points + [1.0]
    values = [legendre_seven(point) for point in points]
    node_count = degree + 1
    weights = np.array([2.0 / (degree * (degree + 1) * value * value) for value in values])
    derivative = np.zeros((node_count, node_count))
    for row_index in range(node_count):
        for col_index in range(node_count):
            if row_index != col_index:
                derivative[row_index, col_index] = values[row_index] / (
                    values[col_index] * (points[row_index] - points[col_index])
                )
    derivative[0, 0] = -degree * (degree + 1) / 4.0
    derivative[node_count - 1, node_count - 1] = degree * (degree + 1) / 4.0
    return derivative, weights


DERIVATIVE, WEIGHTS = gll_tables()
WEIGHTS = [float(w) for w in WEIGHTS]


def halves(matrix):
    plus = [[float(0.5 * (matrix[a, b] - matrix[a, 7 - b])) for b in range(4)] for a in range(4)]
    minus = [[float(0.5 * (matrix[a, b] + matrix[a, 7 - b])) for b in range(4)] for a in range(4)]
    return plus, minus


GRAD = halves(DERIVATIVE)
BACK = halves(DERIVATIVE.T)
BACK_X = halves(DERIVATIVE.T * np.array(WEIGHTS)[None, :])


def apply_halves(tables, planes):
    plus, minus = tables
    diff = [planes[b] - planes[7 - b] for b in range(4)]
    total = [planes[b] + planes[7 - b] for b in range(4)]
    out = [None] * 8
    for a in range(4):
        p = plus[a][0] * diff[0]
        q = minus[a][0] * total[0]
        for b in range(1, 4):
            p = p + plus[a][b] * diff[b]
            q = q + minus[a][b] * total[b]
        out[a] = p + q
        out[7 - a] = p - q
    return out


def lane_table(matrix):
    full = np.kron(np.eye(16), matrix).astype(np.float32)
    high = full.astype(BF16).astype(np.float32)
    row = np.concatenate([high, full - high], axis=1)
    return np.concatenate([row, row], axis=0).astype(BF16)


def lane_apply(rows, table):
    high = rows.astype(BF16)
    low = (rows - high.astype(F32)).astype(BF16)
    both = jnp.dot(jnp.concatenate([high, low], axis=1), table, preferred_element_type=F32)
    return both[:, :LANES] + both[:, LANES:]


def weight_vector(index):
    out = jnp.full(index.shape, WEIGHTS[0], F32)
    for i in range(1, 8):
        out = jnp.where(index % 8 == i, WEIGHTS[i], out)
    return out


def exchange_kernel(
    sizes,
    u_hbm, g_ref, tables_hbm, o_ref,
    u_t, l_t, tab, geo, s_gy, s_gz, s_fy, s_fz,
    xf, yf, rx, ry, zr, edge, edge_y, edge_x, send_y, send_x,
    in_sem, tab_sem, xs, xr, ys, yr, zs, zrs, eys, eyr, exs, exr,
):
    nx, ny, nz = sizes
    ix, iy, iz = lax.axis_index("gx"), lax.axis_index("gy"), lax.axis_index("gz")
    parity = iy % 2
    has_x = [ix > 0, ix < nx - 1]
    has_y = [iy > 0, iy < ny - 1]
    has_z = [iz > 0, iz < nz - 1]
    no_x = [ix == 0, ix == nx - 1]
    no_y = [iy == 0, iy == ny - 1]
    step_of = [-1, 1]

    def load(t):
        return pltpu.make_async_copy(
            u_hbm.at[:, pl.ds(pl.multiple_of(t * LANES, LANES), LANES)], u_t.at[t], in_sem.at[t]
        )

    tile_order = [4, 5, 6, 7, 0, 15, 8, 9, 10, 11, 1, 2, 3, 12, 13, 14]
    table_copy = pltpu.make_async_copy(tables_hbm, tab, tab_sem)
    load(tile_order[0]).start()
    table_copy.start()
    for t in tile_order[1:]:
        load(t).start()

    barrier = pltpu.get_barrier_semaphore()
    dxm = 2 * parity - 1
    mid_x = [(parity == s) & has_x[s] for s in range(2)]
    greet = []
    for s in range(2):
        greet.append((has_x[s], {"gx": ix + step_of[s]}))
        greet.append((has_y[s], {"gy": iy + step_of[s]}))
        greet.append((has_z[s], {"gz": iz + step_of[s]}))
        for r in range(2):
            greet.append((mid_x[s] & has_y[r], {"gx": ix + step_of[s], "gy": iy + step_of[r]}))
    for there, device in greet:

        @pl.when(there)
        def _(device=device):
            pl.semaphore_signal(barrier, inc=1, device_id=device, device_id_type=MESH)

    sub = lax.broadcasted_iota(jnp.int32, (8, LANES), 0)
    lane = lax.broadcasted_iota(jnp.int32, (8, LANES), 1)
    plane_weight = weight_vector(sub) * weight_vector(lane)
    for half in range(2):
        for k in range(6):
            row = jnp.broadcast_to(g_ref[k, 0, :, half * LANES:(half + 1) * LANES], (8, LANES))
            for j in range(8):
                picked = jnp.take_along_axis(row, lane // 8 + 16 * j, axis=1)
                geo[half * 8 + j, 8 * k:8 * k + 8, :] = picked * plane_weight

    for s in range(2):

        @pl.when(no_x[s])
        def _(s=s):
            rx[s] = jnp.zeros(rx.shape[1:], F32)

        @pl.when(no_y[s])
        def _(s=s):
            ry[s] = jnp.zeros(ry.shape[1:], F32)

        for r in range(2):
            corner = 2 * s + r

            @pl.when(no_y[r])
            def _(corner=corner):
                edge_y[corner] = jnp.zeros(edge_y.shape[1:], F32)

            @pl.when(no_x[s] | ((parity != s) & has_y[r]))
            def _(corner=corner):
                edge_x[corner] = jnp.zeros(edge_x.shape[1:], F32)

    def compute(t):
        s_gz[...] = lane_apply(u_t[t], tab[0])
        for c in range(3):
            base = 64 * c
            uy = [u_t[t, pl.ds(base + y, 8, stride=8), :] for y in range(8)]
            gy = apply_halves(GRAD, uy)
            for y in range(8):
                s_gy[pl.ds(base + y, 8, stride=8), :] = gy[y]
        g00, g11, g22, g01, g02, g12 = [geo[t, 8 * k:8 * k + 8, :] for k in range(6)]
        for c in range(3):
            base = 64 * c
            ux = [u_t[t, base + 8 * x:base + 8 * x + 8, :] for x in range(8)]
            gx = apply_halves(GRAD, ux)
            fx = []
            for x in range(8):
                rows = slice(base + 8 * x, base + 8 * x + 8)
                a, b, d = gx[x], s_gy[rows, :], s_gz[rows, :]
                fx.append(g00 * a + g01 * b + g02 * d)
                s_fy[rows, :] = g01 * a + g11 * b + g12 * d
                s_fz[rows, :] = g02 * a + g12 * b + g22 * d
            ox = apply_halves(BACK_X, fx)
            for x in range(8):
                l_t[t, base + 8 * x:base + 8 * x + 8, :] = ox[x]
        s_gz[...] = lane_apply(s_fz[...], tab[1])
        for c in range(3):
            base = 64 * c
            fy = [s_fy[pl.ds(base + y, 8, stride=8), :] for y in range(8)]
            oy = apply_halves(BACK, fy)
            for y in range(8):
                s_gy[pl.ds(base + y, 8, stride=8), :] = oy[y]
        for c in range(3):
            base = 64 * c
            for x in range(8):
                rows = slice(base + 8 * x, base + 8 * x + 8)
                l_t[t, rows, :] = l_t[t, rows, :] + WEIGHTS[x] * (s_gy[rows, :] + s_gz[rows, :])

    def faces(t):
        ch, tt = t // 4, t % 4
        for c in range(3):
            at = pl.ds(4 + 4 * c + tt, 8, stride=12)
            for s in range(2):
                first = 64 * c + 56 * s
                xf[s, ch, at, :] = l_t[t, first:first + 8, :]
                yf[s, ch, at, :] = l_t[t, pl.ds(64 * c + 7 * s, 8, stride=8), :]

    body = pl.ds(16, 72)

    def face_copy(buf, land, send, recv, axis, index, s, ch):
        return pltpu.make_async_remote_copy(
            src_ref=buf.at[s, ch, body], dst_ref=land.at[1 - s, ch, body],
            send_sem=send.at[s, ch], recv_sem=recv.at[1 - s, ch],
            device_id={axis: index + step_of[s]}, device_id_type=MESH,
        )

    def x_copy(s, ch):
        return face_copy(xf, rx, xs, xr, "gx", ix, s, ch)

    def y_copy(s, ch):
        return face_copy(yf, ry, ys, yr, "gy", iy, s, ch)

    def send_faces(ch):
        for s in range(2):

            @pl.when(has_x[s])
            def _(s=s):
                x_copy(s, ch).start()

            @pl.when(has_y[s])
            def _(s=s):
                y_copy(s, ch).start()

    def z_copy(s):
        return pltpu.make_async_remote_copy(
            src_ref=l_t.at[15 * s], dst_ref=zr.at[1 - s], send_sem=zs.at[s], recv_sem=zrs.at[1 - s],
            device_id={"gz": iz + step_of[s]}, device_id_type=MESH,
        )

    table_copy.wait()

    def step(i, carry):
        t = jnp.where(
            i < 4, i + 4,
            jnp.where(i < 6, (i - 4) * 15, jnp.where(i < 10, i + 2, jnp.where(i < 13, i - 9, i - 1))),
        )
        load(t).wait()
        compute(t)
        faces(t)

        @pl.when(i == 3)
        def _():
            pl.semaphore_wait(barrier, sum(there.astype(jnp.int32) for there, _ in greet))
            send_faces(1)

        @pl.when(i == 5)
        def _():
            for s in range(2):

                @pl.when(has_z[s])
                def _(s=s):
                    z_copy(s).start()

        return carry

    lax.fori_loop(0, 16, step, 0)

    wide = lax.broadcasted_iota(jnp.int32, (192, LANES), 1)
    for s in range(2):

        @pl.when(has_z[s])
        def _(s=s):
            z_copy(s).wait_send()
            z_copy(1 - s).wait_recv()
            landed = pltpu.roll(zr[s], 1 if s == 0 else LANES - 1, 1)
            l_t[15 * s] = l_t[15 * s] + jnp.where(wide == (LANES - 1) * s, landed, 0.0)
            faces(15 * s)

    for s in range(2):
        for r in range(2):
            for ch in range(4):
                first = 4 + 84 * r
                edge[2 * s + r, 12 * ch:12 * ch + 12, :] = xf[s, ch, first:first + 12, :]

    def along_y(s, r, buf):
        k, there = 2 * s + r, 2 * s + 1 - r
        return pltpu.make_async_remote_copy(
            src_ref=buf.at[k], dst_ref=edge_y.at[there], send_sem=eys.at[k], recv_sem=eyr.at[there],
            device_id={"gy": iy + step_of[r]}, device_id_type=MESH,
        )

    def along_x(s, r, buf, diagonal):
        k, there = 2 * s + r, 2 * (1 - s) + (1 - r if diagonal else r)
        device = {"gx": ix + step_of[s]}
        if diagonal:
            device["gy"] = iy + step_of[r]
        return pltpu.make_async_remote_copy(
            src_ref=buf.at[k], dst_ref=edge_x.at[there], send_sem=exs.at[k], recv_sem=exr.at[there],
            device_id=device, device_id_type=MESH,
        )

    corners = [(s, r) for s in range(2) for r in range(2)]
    middle = {(s, r): mid_x[s] & has_y[r] for s, r in corners}
    ends = {(s, r): has_y[r] & ((parity != s) | no_x[s]) for s, r in corners}
    alone = {(s, r): has_x[s] & no_y[r] for s, r in corners}

    for s, r in corners:

        @pl.when(ends[s, r])
        def _(s=s, r=r):
            along_y(s, r, edge).start()

        @pl.when(alone[s, r])
        def _(s=s, r=r):
            along_x(s, r, edge, False).start()

    send_faces(2)

    def arrived_y(s, r):
        along_y(s, 1 - r, edge).wait_recv()

    def arrived_x(s, r):
        along_x(1 - s, 1 - r, edge, True).wait_recv()

    for s, r in corners:

        @pl.when(middle[s, r])
        def _(s=s, r=r):
            k = 2 * s + r
            arrived_y(s, r)
            send_x[k] = edge_y[k] + edge[k]
            along_x(s, r, send_x, True).start()

    send_faces(0)

    for s, r in corners:

        @pl.when(middle[s, r])
        def _(s=s, r=r):
            k = 2 * s + r
            arrived_x(s, r)
            send_y[k] = edge_x[k] + edge[k]
            along_y(s, r, send_y).start()

    send_faces(3)

    for s, r in corners:

        @pl.when(ends[s, r])
        def _(s=s, r=r):
            arrived_y(s, r)

        @pl.when(alone[s, r])
        def _(s=s, r=r):
            arrived_x(s, r)

    transverse = lax.broadcasted_iota(jnp.int32, (8, LANES), 0)
    inner = (transverse > 0) & (transverse < 7)

    def finish(ch):
        for s in range(2):

            @pl.when(has_x[s])
            def _(s=s):
                x_copy(1 - s, ch).wait_recv()

            @pl.when(has_y[s])
            def _(s=s):
                y_copy(1 - s, ch).wait_recv()

        for s, r in corners:
            k, first = 2 * s + r, 4 + 84 * r
            part = slice(12 * ch, 12 * ch + 12)
            rx[s, ch, first:first + 12, :] = edge_y[k, part, :] + edge_x[k, part, :]

        def tile(tt, carry):
            t = 4 * ch + tt
            lanes = pl.ds(pl.multiple_of(t * LANES, LANES), LANES)
            for c in range(3):
                at = pl.ds(4 + 4 * c + tt, 8, stride=12)
                for s in range(2):
                    rows = slice(64 * c + 56 * s, 64 * c + 56 * s + 8)
                    l_t[t, rows, :] = l_t[t, rows, :] + rx[s, ch, at, :]
                for s in range(2):
                    rows = pl.ds(64 * c + 7 * s, 8, stride=8)
                    l_t[t, rows, :] = l_t[t, rows, :] + jnp.where(inner, ry[s, ch, at, :], 0.0)
            o_ref[:, lanes] = l_t[t]
            return carry

        lax.fori_loop(0, 4, tile, 0)

    for ch in (1, 2, 0, 3):
        finish(ch)

    for s in range(2):
        for ch in range(4):

            @pl.when(has_x[s])
            def _(s=s, ch=ch):
                x_copy(s, ch).wait_send()

            @pl.when(has_y[s])
            def _(s=s, ch=ch):
                y_copy(s, ch).wait_send()

    for s, r in corners:

        @pl.when(has_y[r])
        def _(s=s, r=r):
            along_y(s, r, edge).wait_send()

        @pl.when(middle[s, r] | alone[s, r])
        def _(s=s, r=r):
            along_x(s, r, edge, True).wait_send()


def third_direction_kernel(x_ref, o_hbm, out, sem):
    lane = lax.broadcasted_iota(jnp.int32, (8, out.shape[1]), 1)
    point = lane % 8
    last = out.shape[1] - 1
    top = (point == 7) & (lane != last)
    bottom = (point == 0) & (lane != 0)

    def copy(i):
        rows = pl.ds(pl.multiple_of(i * 8, 8), 8)
        return pltpu.make_async_copy(out.at[rows], o_hbm.at[rows], sem.at[i])

    def step(i, carry):
        rows = pl.ds(pl.multiple_of(i * 8, 8), 8)
        v = x_ref[rows, :]
        above = pltpu.roll(v, last, 1)
        below = pltpu.roll(v, 1, 1)
        out[rows, :] = v + jnp.where(top, above, jnp.where(bottom, below, 0.0))
        copy(i).start()
        return carry

    count = out.shape[0] // 8
    lax.fori_loop(0, count, step, 0)

    def drain(i, carry):
        copy(i).wait()
        return carry

    lax.fori_loop(0, count, drain, 0)


def solution(mesh):
    sizes = (mesh.shape["gx"], mesh.shape["gy"], mesh.shape["gz"])

    def local(values, geometry):
        tables = jnp.asarray(np.stack([lane_table(DERIVATIVE.T), lane_table(DERIVATIVE)]))
        rows, length = 192, values.shape[3]
        vmem = pl.BlockSpec(memory_space=pltpu.VMEM)
        anywhere = pl.BlockSpec(memory_space=pl.ANY)
        dma = pltpu.SemaphoreType.DMA
        summed = pl.pallas_call(
            functools.partial(exchange_kernel, sizes),
            name="exchange",
            out_shape=jax.ShapeDtypeStruct((rows, length), F32),
            in_specs=[anywhere, vmem, anywhere],
            out_specs=vmem,
            scratch_shapes=[
                pltpu.VMEM((16, rows, LANES), F32),
                pltpu.VMEM((16, rows, LANES), F32),
                pltpu.VMEM((2, 256, 256), BF16),
                pltpu.VMEM((16, 48, LANES), F32),
            ]
            + [pltpu.VMEM((rows, LANES), F32)] * 4
            + [pltpu.VMEM((2, 4, 104, LANES), F32)] * 4
            + [pltpu.VMEM((2, rows, LANES), F32)]
            + [pltpu.VMEM((4, 48, LANES), F32)] * 5
            + [dma((16,)), dma(())]
            + [dma((2, 4))] * 4
            + [dma((2,))] * 2
            + [dma((4,))] * 4,
            compiler_params=pltpu.CompilerParams(collective_id=0, has_side_effects=True),
        )(values.reshape(rows, length), geometry, tables)
        out = pl.pallas_call(
            third_direction_kernel,
            name="third",
            out_shape=jax.ShapeDtypeStruct((rows, length), F32),
            in_specs=[vmem],
            out_specs=anywhere,
            scratch_shapes=[pltpu.VMEM((rows, length), F32), dma((rows // 8,))],
        )(summed)
        return out.reshape(values.shape)

    return jax.shard_map(
        local,
        mesh=mesh,
        in_specs=(P(None, "gx", "gy", "gz"), P(None, "gx", "gy", "gz")),
        out_specs=P(None, "gx", "gy", "gz"),
        check_vma=False,
    )
```

```python
import functools

import jax
import jax.numpy as jnp
import numpy as np
from jax import lax
from jax.experimental import pallas as pl
from jax.experimental.pallas import tpu as pltpu
from jax.sharding import PartitionSpec as P

MESH = pl.DeviceIdType.MESH
F32 = jnp.float32
BF16 = jnp.bfloat16
LANES = 128

interior_points = [
    -0.8717401485096066,
    -0.5917001814331423,
    -0.2092992179024789,
    0.2092992179024789,
    0.5917001814331423,
    0.8717401485096066,
]


def legendre_seven(point):
    previous = 1.0
    current = point
    for order in range(1, 7):
        following = ((2 * order + 1) * point * current - order * previous) / (order + 1)
        previous = current
        current = following
    return current


def gll_tables():
    degree = 7
    points = [-1.0] + interior_points + [1.0]
    values = [legendre_seven(point) for point in points]
    node_count = degree + 1
    weights = np.array([2.0 / (degree * (degree + 1) * value * value) for value in values])
    derivative = np.zeros((node_count, node_count))
    for row_index in range(node_count):
        for col_index in range(node_count):
            if row_index != col_index:
                derivative[row_index, col_index] = values[row_index] / (
                    values[col_index] * (points[row_index] - points[col_index])
                )
    derivative[0, 0] = -degree * (degree + 1) / 4.0
    derivative[node_count - 1, node_count - 1] = degree * (degree + 1) / 4.0
    return derivative, weights


DERIVATIVE, WEIGHTS = gll_tables()
WEIGHTS = [float(w) for w in WEIGHTS]


def halves(matrix):
    plus = [[float(0.5 * (matrix[a, b] - matrix[a, 7 - b])) for b in range(4)] for a in range(4)]
    minus = [[float(0.5 * (matrix[a, b] + matrix[a, 7 - b])) for b in range(4)] for a in range(4)]
    return plus, minus


GRAD = halves(DERIVATIVE)
BACK = halves(DERIVATIVE.T)
BACK_X = halves(DERIVATIVE.T * np.array(WEIGHTS)[None, :])


def apply_halves(tables, planes):
    plus, minus = tables
    diff = [planes[b] - planes[7 - b] for b in range(4)]
    total = [planes[b] + planes[7 - b] for b in range(4)]
    out = [None] * 8
    for a in range(4):
        p = plus[a][0] * diff[0]
        q = minus[a][0] * total[0]
        for b in range(1, 4):
            p = p + plus[a][b] * diff[b]
            q = q + minus[a][b] * total[b]
        out[a] = p + q
        out[7 - a] = p - q
    return out


def lane_table(matrix):
    full = np.kron(np.eye(16), matrix).astype(np.float32)
    high = full.astype(BF16).astype(np.float32)
    row = np.concatenate([high, full - high], axis=1)
    return np.concatenate([row, row], axis=0).astype(BF16)


def lane_apply(rows, table):
    high = rows.astype(BF16)
    low = (rows - high.astype(F32)).astype(BF16)
    both = jnp.dot(jnp.concatenate([high, low], axis=1), table, preferred_element_type=F32)
    return both[:, :LANES] + both[:, LANES:]


def weight_vector(index):
    out = jnp.full(index.shape, WEIGHTS[0], F32)
    for i in range(1, 8):
        out = jnp.where(index % 8 == i, WEIGHTS[i], out)
    return out


def exchange_kernel(
    sizes,
    u_hbm, g_hbm, tables_hbm, o_ref,
    g_ref, u_t, l_t, tab, geo, s_gy, s_gz, s_fy, s_fz,
    xf, yf, rx, ry, zr, edge, edge_y, edge_x, edge_d, send_y,
    g_sem, in_sem, tab_sem, xs, xr, ys, yr, zs, zrs, eys, eyr, exs, exr, eds, edr,
):
    nx, ny, nz = sizes
    ix, iy, iz = lax.axis_index("gx"), lax.axis_index("gy"), lax.axis_index("gz")
    parity = iy % 2
    has_x = [ix > 0, ix < nx - 1]
    has_y = [iy > 0, iy < ny - 1]
    has_z = [iz > 0, iz < nz - 1]
    no_x = [ix == 0, ix == nx - 1]
    no_y = [iy == 0, iy == ny - 1]
    step_of = [-1, 1]

    def load(t):
        return pltpu.make_async_copy(
            u_hbm.at[:, pl.ds(pl.multiple_of(t * LANES, LANES), LANES)], u_t.at[t], in_sem.at[t]
        )

    tile_order = [4, 5, 6, 7, 0, 15, 8, 9, 10, 11, 1, 2, 3, 12, 13, 14]
    table_copy = pltpu.make_async_copy(tables_hbm, tab, tab_sem)
    geometry_copy = pltpu.make_async_copy(g_hbm, g_ref, g_sem)
    geometry_copy.start()
    load(tile_order[0]).start()
    table_copy.start()
    for t in tile_order[1:]:
        load(t).start()

    barrier = pltpu.get_barrier_semaphore()
    dxm = 2 * parity - 1
    mid_x = [(parity == s) & has_x[s] for s in range(2)]
    greet = []
    for s in range(2):
        greet.append((has_x[s], {"gx": ix + step_of[s]}))
        greet.append((has_y[s], {"gy": iy + step_of[s]}))
        greet.append((has_z[s], {"gz": iz + step_of[s]}))
        for r in range(2):
            greet.append((mid_x[s] & has_y[r], {"gx": ix + step_of[s], "gy": iy + step_of[r]}))
    for there, device in greet:

        @pl.when(there)
        def _(device=device):
            pl.semaphore_signal(barrier, inc=1, device_id=device, device_id_type=MESH)

    sub = lax.broadcasted_iota(jnp.int32, (8, LANES), 0)
    lane = lax.broadcasted_iota(jnp.int32, (8, LANES), 1)
    plane_weight = weight_vector(sub) * weight_vector(lane)
    geometry_copy.wait()
    for half in range(2):
        for k in range(6):
            row = jnp.broadcast_to(g_ref[k, 0, :, half * LANES:(half + 1) * LANES], (8, LANES))
            for j in range(8):
                picked = jnp.take_along_axis(row, lane // 8 + 16 * j, axis=1)
                geo[half * 8 + j, 8 * k:8 * k + 8, :] = picked * plane_weight

    for s in range(2):

        @pl.when(no_x[s])
        def _(s=s):
            rx[s] = jnp.zeros(rx.shape[1:], F32)

        @pl.when(no_y[s])
        def _(s=s):
            ry[s] = jnp.zeros(ry.shape[1:], F32)

        for r in range(2):
            corner = 2 * s + r

            @pl.when(no_y[r])
            def _(corner=corner):
                edge_y[corner] = jnp.zeros(edge_y.shape[1:], F32)

            @pl.when(no_x[s] | ((parity != s) & has_y[r]))
            def _(corner=corner):
                edge_x[corner] = jnp.zeros(edge_x.shape[1:], F32)

            @pl.when(no_x[s] | (parity != s) | no_y[r])
            def _(corner=corner):
                edge_d[corner] = jnp.zeros(edge_d.shape[1:], F32)

    def compute(t):
        s_gz[...] = lane_apply(u_t[t], tab[0])
        for c in range(3):
            base = 64 * c
            uy = [u_t[t, pl.ds(base + y, 8, stride=8), :] for y in range(8)]
            gy = apply_halves(GRAD, uy)
            for y in range(8):
                s_gy[pl.ds(base + y, 8, stride=8), :] = gy[y]
        g00, g11, g22, g01, g02, g12 = [geo[t, 8 * k:8 * k + 8, :] for k in range(6)]
        for c in range(3):
            base = 64 * c
            ux = [u_t[t, base + 8 * x:base + 8 * x + 8, :] for x in range(8)]
            gx = apply_halves(GRAD, ux)
            fx = []
            for x in range(8):
                rows = slice(base + 8 * x, base + 8 * x + 8)
                a, b, d = gx[x], s_gy[rows, :], s_gz[rows, :]
                fx.append(g00 * a + g01 * b + g02 * d)
                s_fy[rows, :] = g01 * a + g11 * b + g12 * d
                s_fz[rows, :] = g02 * a + g12 * b + g22 * d
            ox = apply_halves(BACK_X, fx)
            for x in range(8):
                l_t[t, base + 8 * x:base + 8 * x + 8, :] = ox[x]
        s_gz[...] = lane_apply(s_fz[...], tab[1])
        for c in range(3):
            base = 64 * c
            fy = [s_fy[pl.ds(base + y, 8, stride=8), :] for y in range(8)]
            oy = apply_halves(BACK, fy)
            for y in range(8):
                s_gy[pl.ds(base + y, 8, stride=8), :] = oy[y]
        for c in range(3):
            base = 64 * c
            for x in range(8):
                rows = slice(base + 8 * x, base + 8 * x + 8)
                l_t[t, rows, :] = l_t[t, rows, :] + WEIGHTS[x] * (s_gy[rows, :] + s_gz[rows, :])

    def faces(t):
        ch, tt = t // 4, t % 4
        for c in range(3):
            at = pl.ds(4 + 4 * c + tt, 8, stride=12)
            for s in range(2):
                first = 64 * c + 56 * s
                xf[s, ch, at, :] = l_t[t, first:first + 8, :]
                yf[s, ch, at, :] = l_t[t, pl.ds(64 * c + 7 * s, 8, stride=8), :]

    body = pl.ds(16, 72)

    def face_copy(buf, land, send, recv, axis, index, s, ch):
        return pltpu.make_async_remote_copy(
            src_ref=buf.at[s, ch, body], dst_ref=land.at[1 - s, ch, body],
            send_sem=send.at[s, ch], recv_sem=recv.at[1 - s, ch],
            device_id={axis: index + step_of[s]}, device_id_type=MESH,
        )

    def x_copy(s, ch):
        return face_copy(xf, rx, xs, xr, "gx", ix, s, ch)

    def y_copy(s, ch):
        return face_copy(yf, ry, ys, yr, "gy", iy, s, ch)

    def send_faces(ch):
        for s in range(2):

            @pl.when(has_x[s])
            def _(s=s):
                x_copy(s, ch).start()

            @pl.when(has_y[s])
            def _(s=s):
                y_copy(s, ch).start()

    def z_copy(s):
        return pltpu.make_async_remote_copy(
            src_ref=l_t.at[15 * s], dst_ref=zr.at[1 - s], send_sem=zs.at[s], recv_sem=zrs.at[1 - s],
            device_id={"gz": iz + step_of[s]}, device_id_type=MESH,
        )

    table_copy.wait()

    def step(i, carry):
        t = jnp.where(
            i < 4, i + 4,
            jnp.where(i < 6, (i - 4) * 15, jnp.where(i < 10, i + 2, jnp.where(i < 13, i - 9, i - 1))),
        )
        load(t).wait()
        compute(t)
        faces(t)

        @pl.when(i == 3)
        def _():
            pl.semaphore_wait(barrier, sum(there.astype(jnp.int32) for there, _ in greet))
            send_faces(1)

        @pl.when(i == 9)
        def _():
            send_faces(2)

        @pl.when(i == 5)
        def _():
            for s in range(2):

                @pl.when(has_z[s])
                def _(s=s):
                    z_copy(s).start()

        return carry

    lax.fori_loop(0, 16, step, 0)

    wide = lax.broadcasted_iota(jnp.int32, (192, LANES), 1)
    for s in range(2):

        @pl.when(has_z[s])
        def _(s=s):
            z_copy(s).wait_send()
            z_copy(1 - s).wait_recv()
            landed = pltpu.roll(zr[s], 1 if s == 0 else LANES - 1, 1)
            l_t[15 * s] = l_t[15 * s] + jnp.where(wide == (LANES - 1) * s, landed, 0.0)
            faces(15 * s)

    for s in range(2):
        for r in range(2):
            for ch in range(4):
                first = 4 + 84 * r
                edge[2 * s + r, 12 * ch:12 * ch + 12, :] = xf[s, ch, first:first + 12, :]

    def along_y(s, r, buf):
        k, there = 2 * s + r, 2 * s + 1 - r
        return pltpu.make_async_remote_copy(
            src_ref=buf.at[k], dst_ref=edge_y.at[there], send_sem=eys.at[k], recv_sem=eyr.at[there],
            device_id={"gy": iy + step_of[r]}, device_id_type=MESH,
        )

    def along_x(s, r):
        k, there = 2 * s + r, 2 * (1 - s) + r
        return pltpu.make_async_remote_copy(
            src_ref=edge.at[k], dst_ref=edge_x.at[there], send_sem=exs.at[k], recv_sem=exr.at[there],
            device_id={"gx": ix + step_of[s]}, device_id_type=MESH,
        )

    def across(s, r):
        k, there = 2 * s + r, 2 * (1 - s) + 1 - r
        return pltpu.make_async_remote_copy(
            src_ref=edge.at[k], dst_ref=edge_d.at[there], send_sem=eds.at[k], recv_sem=edr.at[there],
            device_id={"gx": ix + step_of[s], "gy": iy + step_of[r]}, device_id_type=MESH,
        )

    corners = [(s, r) for s in range(2) for r in range(2)]
    inner_one = {(s, r): mid_x[s] & has_y[r] for s, r in corners}
    outer_one = {(s, r): has_y[r] & ((parity != s) | no_x[s]) for s, r in corners}
    alone = {(s, r): has_x[s] & no_y[r] for s, r in corners}
    send_x = {(s, r): has_x[s] & (no_y[r] | (parity != s)) for s, r in corners}

    for s, r in corners:

        @pl.when(outer_one[s, r])
        def _(s=s, r=r):
            along_y(s, r, edge).start()

        @pl.when(send_x[s, r])
        def _(s=s, r=r):
            along_x(s, r).start()

        @pl.when(inner_one[s, r])
        def _(s=s, r=r):
            across(s, r).start()

    send_faces(0)

    for s, r in corners:

        @pl.when(inner_one[s, r])
        def _(s=s, r=r):
            k = 2 * s + r
            along_x(1 - s, r).wait_recv()
            across(1 - s, 1 - r).wait_recv()
            send_y[k] = edge_x[k] + edge_d[k] + edge[k]
            along_y(s, r, send_y).start()

    send_faces(3)

    for s, r in corners:

        @pl.when(has_y[r])
        def _(s=s, r=r):
            along_y(s, 1 - r, edge).wait_recv()

        @pl.when(alone[s, r])
        def _(s=s, r=r):
            along_x(1 - s, r).wait_recv()

    transverse = lax.broadcasted_iota(jnp.int32, (8, LANES), 0)
    inner = (transverse > 0) & (transverse < 7)

    def finish(ch):
        for s in range(2):

            @pl.when(has_x[s])
            def _(s=s):
                x_copy(1 - s, ch).wait_recv()

            @pl.when(has_y[s])
            def _(s=s):
                y_copy(1 - s, ch).wait_recv()

        for s, r in corners:
            k, first = 2 * s + r, 4 + 84 * r
            part = slice(12 * ch, 12 * ch + 12)
            rx[s, ch, first:first + 12, :] = edge_y[k, part, :] + edge_x[k, part, :] + edge_d[k, part, :]

        def tile(tt, carry):
            t = 4 * ch + tt
            lanes = pl.ds(pl.multiple_of(t * LANES, LANES), LANES)
            for c in range(3):
                at = pl.ds(4 + 4 * c + tt, 8, stride=12)
                for s in range(2):
                    rows = slice(64 * c + 56 * s, 64 * c + 56 * s + 8)
                    l_t[t, rows, :] = l_t[t, rows, :] + rx[s, ch, at, :]
                for s in range(2):
                    rows = pl.ds(64 * c + 7 * s, 8, stride=8)
                    l_t[t, rows, :] = l_t[t, rows, :] + jnp.where(inner, ry[s, ch, at, :], 0.0)
            o_ref[:, lanes] = l_t[t]
            return carry

        lax.fori_loop(0, 4, tile, 0)

    for ch in (1, 2, 0, 3):
        finish(ch)

    for s in range(2):
        for ch in range(4):

            @pl.when(has_x[s])
            def _(s=s, ch=ch):
                x_copy(s, ch).wait_send()

            @pl.when(has_y[s])
            def _(s=s, ch=ch):
                y_copy(s, ch).wait_send()

    for s, r in corners:

        @pl.when(has_y[r])
        def _(s=s, r=r):
            along_y(s, r, edge).wait_send()

        @pl.when(send_x[s, r])
        def _(s=s, r=r):
            along_x(s, r).wait_send()

        @pl.when(inner_one[s, r])
        def _(s=s, r=r):
            across(s, r).wait_send()


def third_direction_kernel(x_ref, o_hbm, out, sem):
    lane = lax.broadcasted_iota(jnp.int32, (8, out.shape[1]), 1)
    point = lane % 8
    last = out.shape[1] - 1
    top = (point == 7) & (lane != last)
    bottom = (point == 0) & (lane != 0)

    def copy(i):
        rows = pl.ds(i * 8 if isinstance(i, int) else pl.multiple_of(i * 8, 8), 8)
        return pltpu.make_async_copy(out.at[rows], o_hbm.at[rows], sem.at[i])

    def step(i, carry):
        rows = pl.ds(i * 8, 8)
        v = x_ref[rows, :]
        above = pltpu.roll(v, last, 1)
        below = pltpu.roll(v, 1, 1)
        out[rows, :] = v + jnp.where(top, above, jnp.where(bottom, below, 0.0))
        copy(i).start()
        return carry

    count = out.shape[0] // 8
    for i in range(count):
        step(i, 0)

    def drain(i, carry):
        copy(i).wait()
        return carry

    lax.fori_loop(0, count, drain, 0)


def solution(mesh):
    sizes = (mesh.shape["gx"], mesh.shape["gy"], mesh.shape["gz"])

    def local(values, geometry):
        tables = jnp.asarray(np.stack([lane_table(DERIVATIVE.T), lane_table(DERIVATIVE)]))
        rows, length = 192, values.shape[3]
        vmem = pl.BlockSpec(memory_space=pltpu.VMEM)
        hbm = pl.BlockSpec(memory_space=pltpu.HBM)
        dma = pltpu.SemaphoreType.DMA
        summed = pl.pallas_call(
            functools.partial(exchange_kernel, sizes),
            name="exchange",
            out_shape=pltpu.VMEM((rows, length), F32),
            in_specs=[hbm, hbm, hbm],
            out_specs=vmem,
            scratch_shapes=[
                pltpu.VMEM(geometry.shape, F32),
                pltpu.VMEM((16, rows, LANES), F32),
                pltpu.VMEM((16, rows, LANES), F32),
                pltpu.VMEM((2, 256, 256), BF16),
                pltpu.VMEM((16, 48, LANES), F32),
            ]
            + [pltpu.VMEM((rows, LANES), F32)] * 4
            + [pltpu.VMEM((2, 4, 104, LANES), F32)] * 4
            + [pltpu.VMEM((2, rows, LANES), F32)]
            + [pltpu.VMEM((4, 48, LANES), F32)] * 5
            + [dma(()), dma((16,)), dma(())]
            + [dma((2, 4))] * 4
            + [dma((2,))] * 2
            + [dma((4,))] * 6,
            compiler_params=pltpu.CompilerParams(collective_id=0, has_side_effects=True, vmem_limit_bytes=16 << 20),
        )(
            pltpu.with_memory_space_constraint(values.reshape(rows, length), pltpu.HBM),
            pltpu.with_memory_space_constraint(geometry, pltpu.HBM),
            pltpu.with_memory_space_constraint(tables, pltpu.HBM),
        )
        out = pl.pallas_call(
            third_direction_kernel,
            name="third",
            out_shape=jax.ShapeDtypeStruct((rows, length), F32),
            in_specs=[vmem],
            out_specs=hbm,
            scratch_shapes=[pltpu.VMEM((rows, length), F32), dma((rows // 8,))],
            compiler_params=pltpu.CompilerParams(vmem_limit_bytes=8 << 20),
        )(summed)
        return out.reshape(values.shape)

    return jax.shard_map(
        local,
        mesh=mesh,
        in_specs=(P(None, "gx", "gy", "gz"), P(None, "gx", "gy", "gz")),
        out_specs=P(None, "gx", "gy", "gz"),
        check_vma=False,
    )
```

```python
import functools

import jax
import jax.numpy as jnp
import numpy as np
from jax import lax
from jax.experimental import pallas as pl
from jax.experimental.pallas import tpu as pltpu
from jax.sharding import PartitionSpec as P

MESH = pl.DeviceIdType.MESH
F32 = jnp.float32
BF16 = jnp.bfloat16
LANES = 128

interior_points = [
    -0.8717401485096066,
    -0.5917001814331423,
    -0.2092992179024789,
    0.2092992179024789,
    0.5917001814331423,
    0.8717401485096066,
]


def legendre_seven(point):
    previous = 1.0
    current = point
    for order in range(1, 7):
        following = ((2 * order + 1) * point * current - order * previous) / (order + 1)
        previous = current
        current = following
    return current


def gll_tables():
    degree = 7
    points = [-1.0] + interior_points + [1.0]
    values = [legendre_seven(point) for point in points]
    node_count = degree + 1
    weights = np.array([2.0 / (degree * (degree + 1) * value * value) for value in values])
    derivative = np.zeros((node_count, node_count))
    for row_index in range(node_count):
        for col_index in range(node_count):
            if row_index != col_index:
                derivative[row_index, col_index] = values[row_index] / (
                    values[col_index] * (points[row_index] - points[col_index])
                )
    derivative[0, 0] = -degree * (degree + 1) / 4.0
    derivative[node_count - 1, node_count - 1] = degree * (degree + 1) / 4.0
    return derivative, weights


DERIVATIVE, WEIGHTS = gll_tables()
WEIGHTS = [float(w) for w in WEIGHTS]


def halves(matrix):
    plus = [[float(0.5 * (matrix[a, b] - matrix[a, 7 - b])) for b in range(4)] for a in range(4)]
    minus = [[float(0.5 * (matrix[a, b] + matrix[a, 7 - b])) for b in range(4)] for a in range(4)]
    return plus, minus


GRAD = halves(DERIVATIVE)
BACK = halves(DERIVATIVE.T)
BACK_X = halves(DERIVATIVE.T * np.array(WEIGHTS)[None, :])


def apply_halves(tables, planes):
    plus, minus = tables
    diff = [planes[b] - planes[7 - b] for b in range(4)]
    total = [planes[b] + planes[7 - b] for b in range(4)]
    out = [None] * 8
    for a in range(4):
        p = plus[a][0] * diff[0]
        q = minus[a][0] * total[0]
        for b in range(1, 4):
            p = p + plus[a][b] * diff[b]
            q = q + minus[a][b] * total[b]
        out[a] = p + q
        out[7 - a] = p - q
    return out


def lane_table(matrix):
    full = np.kron(np.eye(16), matrix).astype(np.float32)
    high = full.astype(BF16).astype(np.float32)
    row = np.concatenate([high, full - high], axis=1)
    return np.concatenate([row, row], axis=0).astype(BF16)


def lane_apply(rows, table):
    high = rows.astype(BF16)
    low = (rows - high.astype(F32)).astype(BF16)
    both = jnp.dot(jnp.concatenate([high, low], axis=1), table, preferred_element_type=F32)
    return both[:, :LANES] + both[:, LANES:]


def weight_vector(index):
    out = jnp.full(index.shape, WEIGHTS[0], F32)
    for i in range(1, 8):
        out = jnp.where(index % 8 == i, WEIGHTS[i], out)
    return out


def exchange_kernel(
    sizes,
    u_hbm, g_hbm, tables_hbm, o_ref,
    g_ref, u_t, l_t, tab, geo, s_gy, s_gz, s_fy, s_fz, s_ox,
    xf, yf, rx, ry, zr, edge, edge_y, edge_x, edge_d, passed,
    g_sem, in_sem, tab_sem, xs, xr, ys, yr, zs, zrs, eys, eyr, exs, exr, eds, edr,
):
    nx, ny, nz = sizes
    ix, iy, iz = lax.axis_index("gx"), lax.axis_index("gy"), lax.axis_index("gz")
    parity = iy % 2
    has_x = [ix > 0, ix < nx - 1]
    has_y = [iy > 0, iy < ny - 1]
    has_z = [iz > 0, iz < nz - 1]
    no_x = [ix == 0, ix == nx - 1]
    no_y = [iy == 0, iy == ny - 1]
    step_of = [-1, 1]

    def load(t):
        return pltpu.make_async_copy(
            u_hbm.at[:, pl.ds(pl.multiple_of(t * LANES, LANES), LANES)], u_t.at[t], in_sem.at[t]
        )

    barrier = pltpu.get_barrier_semaphore()
    dxm = 2 * parity - 1
    mid_x = [(parity == s) & has_x[s] for s in range(2)]
    greet = []
    for s in range(2):
        greet.append((has_x[s], {"gx": ix + step_of[s]}))
        greet.append((has_y[s], {"gy": iy + step_of[s]}))
        greet.append((has_z[s], {"gz": iz + step_of[s]}))
        for r in range(2):
            greet.append((mid_x[s] & has_y[r], {"gx": ix + step_of[s], "gy": iy + step_of[r]}))
    for there, device in greet:

        @pl.when(there)
        def _(device=device):
            pl.semaphore_signal(barrier, inc=1, device_id=device, device_id_type=MESH)

    tile_order = [4, 5, 6, 7, 0, 15, 8, 9, 10, 11, 1, 2, 3, 12, 13, 14]
    table_copy = pltpu.make_async_copy(tables_hbm, tab, tab_sem)
    geometry_copy = pltpu.make_async_copy(g_hbm, g_ref, g_sem)
    geometry_copy.start()
    load(tile_order[0]).start()
    table_copy.start()
    for t in tile_order[1:]:
        load(t).start()

    sub = lax.broadcasted_iota(jnp.int32, (8, LANES), 0)
    lane = lax.broadcasted_iota(jnp.int32, (8, LANES), 1)
    plane_weight = weight_vector(sub) * weight_vector(lane)
    geometry_copy.wait()
    for half in range(2):
        for k in range(6):
            row = jnp.broadcast_to(g_ref[k, 0, :, half * LANES:(half + 1) * LANES], (8, LANES))
            for j in range(8):
                picked = jnp.take_along_axis(row, lane // 8 + 16 * j, axis=1)
                geo[half * 8 + j, 8 * k:8 * k + 8, :] = picked * plane_weight

    for s in range(2):

        @pl.when(no_x[s])
        def _(s=s):
            rx[s] = jnp.zeros(rx.shape[1:], F32)

        @pl.when(no_y[s])
        def _(s=s):
            ry[s] = jnp.zeros(ry.shape[1:], F32)

        for r in range(2):
            corner = 2 * s + r

            @pl.when(no_y[r])
            def _(corner=corner):
                edge_y[corner] = jnp.zeros(edge_y.shape[1:], F32)

            @pl.when(no_x[s] | ((parity != s) & has_y[r]))
            def _(corner=corner):
                edge_x[corner] = jnp.zeros(edge_x.shape[1:], F32)

            @pl.when(no_x[s] | (parity != s) | no_y[r])
            def _(corner=corner):
                edge_d[corner] = jnp.zeros(edge_d.shape[1:], F32)

    def compute(pair):
        for p, t in enumerate(pair):
            s_gz[p] = lane_apply(u_t[t], tab[0])
        for p, t in enumerate(pair):
            for c in range(3):
                uy = [u_t[t, pl.ds(64 * c + y, 8, stride=8), :] for y in range(8)]
                gy = apply_halves(GRAD, uy)
                for y in range(8):
                    s_gy[p, pl.ds(64 * c + y, 8, stride=8), :] = gy[y]
        for p, t in enumerate(pair):
            g00, g11, g22, g01, g02, g12 = [geo[t, 8 * k:8 * k + 8, :] for k in range(6)]
            for c in range(3):
                base = 64 * c
                ux = [u_t[t, base + 8 * x:base + 8 * x + 8, :] for x in range(8)]
                gx = apply_halves(GRAD, ux)
                fx = []
                for x in range(8):
                    rows = slice(base + 8 * x, base + 8 * x + 8)
                    a, b, d = gx[x], s_gy[p, rows, :], s_gz[p, rows, :]
                    fx.append(g00 * a + g01 * b + g02 * d)
                    s_fy[p, rows, :] = g01 * a + g11 * b + g12 * d
                    s_fz[p, rows, :] = g02 * a + g12 * b + g22 * d
                ox = apply_halves(BACK_X, fx)
                for x in range(8):
                    s_ox[p, base + 8 * x:base + 8 * x + 8, :] = ox[x]
            s_gz[p] = lane_apply(s_fz[p], tab[1])
        for p, t in enumerate(pair):
            for c in range(3):
                fy = [s_fy[p, pl.ds(64 * c + y, 8, stride=8), :] for y in range(8)]
                oy = apply_halves(BACK, fy)
                for y in range(8):
                    s_gy[p, pl.ds(64 * c + y, 8, stride=8), :] = oy[y]
        for p, t in enumerate(pair):
            for c in range(3):
                for x in range(8):
                    rows = slice(64 * c + 8 * x, 64 * c + 8 * x + 8)
                    l_t[t, rows, :] = s_ox[p, rows, :] + WEIGHTS[x] * (s_gy[p, rows, :] + s_gz[p, rows, :])

    def faces(t):
        ch, tt = t // 4, t % 4
        for c in range(3):
            at = pl.ds(4 + 4 * c + tt, 8, stride=12)
            for s in range(2):
                first = 64 * c + 56 * s
                xf[s, ch, at, :] = l_t[t, first:first + 8, :]
                yf[s, ch, at, :] = l_t[t, pl.ds(64 * c + 7 * s, 8, stride=8), :]

    body = pl.ds(16, 72)

    def face_copy(buf, land, send, recv, axis, index, s, ch):
        return pltpu.make_async_remote_copy(
            src_ref=buf.at[s, ch, body], dst_ref=land.at[1 - s, ch, body],
            send_sem=send.at[s, ch], recv_sem=recv.at[1 - s, ch],
            device_id={axis: index + step_of[s]}, device_id_type=MESH,
        )

    def x_copy(s, ch):
        return face_copy(xf, rx, xs, xr, "gx", ix, s, ch)

    def y_copy(s, ch):
        return face_copy(yf, ry, ys, yr, "gy", iy, s, ch)

    def send_x(s, ch):
        @pl.when(has_x[s])
        def _():
            x_copy(s, ch).start()

    def send_y(s, ch):
        @pl.when(has_y[s])
        def _():
            y_copy(s, ch).start()

    def z_copy(s):
        return pltpu.make_async_remote_copy(
            src_ref=l_t.at[15 * s], dst_ref=zr.at[1 - s], send_sem=zs.at[s], recv_sem=zrs.at[1 - s],
            device_id={"gz": iz + step_of[s]}, device_id_type=MESH,
        )

    table_copy.wait()

    def step(i, carry):
        first = jnp.where(i < 2, 2 * i + 4, jnp.where(i == 2, 0, jnp.where(i < 5, 2 * i + 2, jnp.where(i < 7, 2 * i - 9, 13))))
        second = jnp.where(i == 2, 15, jnp.where(i == 6, 12, first + 1))
        for t in (first, second):
            load(t).wait()
        compute((first, second))
        for t in (first, second):
            faces(t)

        @pl.when(i == 1)
        def _():
            pl.semaphore_wait(barrier, sum(there.astype(jnp.int32) for there, _ in greet))
            send_x(0, 1)
            send_y(0, 1)
            send_y(1, 1)
            send_x(1, 1)

        @pl.when(i == 4)
        def _():
            send_x(0, 2)
            send_y(0, 2)
            send_y(1, 2)
            send_x(1, 2)

        @pl.when(i == 2)
        def _():
            for s in range(2):

                @pl.when(has_z[s])
                def _(s=s):
                    z_copy(s).start()

        return carry

    lax.fori_loop(0, 8, step, 0)

    wide = lax.broadcasted_iota(jnp.int32, (192, LANES), 1)
    for s in range(2):

        @pl.when(has_z[s])
        def _(s=s):
            z_copy(s).wait_send()
            z_copy(1 - s).wait_recv()
            landed = pltpu.roll(zr[s], 1 if s == 0 else LANES - 1, 1)
            l_t[15 * s] = l_t[15 * s] + jnp.where(wide == (LANES - 1) * s, landed, 0.0)
            faces(15 * s)

    for s in range(2):
        for r in range(2):
            for ch in range(4):
                first = 4 + 84 * r
                edge[2 * s + r, 12 * ch:12 * ch + 12, :] = xf[s, ch, first:first + 12, :]

    def along_y(s, r, buf):
        k, there = 2 * s + r, 2 * s + 1 - r
        return pltpu.make_async_remote_copy(
            src_ref=buf.at[k], dst_ref=edge_y.at[there], send_sem=eys.at[k], recv_sem=eyr.at[there],
            device_id={"gy": iy + step_of[r]}, device_id_type=MESH,
        )

    def along_x(s, r):
        k, there = 2 * s + r, 2 * (1 - s) + r
        return pltpu.make_async_remote_copy(
            src_ref=edge.at[k], dst_ref=edge_x.at[there], send_sem=exs.at[k], recv_sem=exr.at[there],
            device_id={"gx": ix + step_of[s]}, device_id_type=MESH,
        )

    def across(s, r):
        k, there = 2 * s + r, 2 * (1 - s) + 1 - r
        return pltpu.make_async_remote_copy(
            src_ref=edge.at[k], dst_ref=edge_d.at[there], send_sem=eds.at[k], recv_sem=edr.at[there],
            device_id={"gx": ix + step_of[s], "gy": iy + step_of[r]}, device_id_type=MESH,
        )

    corners = [(s, r) for s in range(2) for r in range(2)]
    inner_one = {(s, r): mid_x[s] & has_y[r] for s, r in corners}
    outer_one = {(s, r): has_y[r] & ((parity != s) | no_x[s]) for s, r in corners}
    alone = {(s, r): has_x[s] & no_y[r] for s, r in corners}
    cross_x = {(s, r): has_x[s] & (no_y[r] | (parity != s)) for s, r in corners}

    transverse = lax.broadcasted_iota(jnp.int32, (8, LANES), 0)
    inner = (transverse > 0) & (transverse < 7)

    def finish(ch):
        for s in range(2):

            @pl.when(has_x[s])
            def _(s=s):
                x_copy(1 - s, ch).wait_recv()

            @pl.when(has_y[s])
            def _(s=s):
                y_copy(1 - s, ch).wait_recv()

        def tile(tt, carry):
            t = 4 * ch + tt
            lanes = pl.ds(pl.multiple_of(t * LANES, LANES), LANES)
            for c in range(3):
                at = pl.ds(4 + 4 * c + tt, 8, stride=12)
                for s in range(2):
                    rows = slice(64 * c + 56 * s, 64 * c + 56 * s + 8)
                    l_t[t, rows, :] = l_t[t, rows, :] + jnp.where(inner, rx[s, ch, at, :], 0.0)
                for s in range(2):
                    rows = pl.ds(64 * c + 7 * s, 8, stride=8)
                    l_t[t, rows, :] = l_t[t, rows, :] + jnp.where(inner, ry[s, ch, at, :], 0.0)
            o_ref[:, lanes] = l_t[t]
            return carry

        lax.fori_loop(0, 4, tile, 0)

    def finish_edges():
        for s, r in corners:
            k, first = 2 * s + r, 4 + 84 * r
            for ch in range(4):
                part = slice(12 * ch, 12 * ch + 12)
                xf[s, ch, first:first + 12, :] = edge_y[k, part, :] + edge_x[k, part, :] + edge_d[k, part, :]

        def rows_of(t):
            for c in range(3):
                at = pl.ds(4 + 4 * c + t % 4, 8, stride=12)
                for s in range(2):
                    rows = slice(64 * c + 56 * s, 64 * c + 56 * s + 8)
                    yield rows, jnp.where(inner, 0.0, xf[s, t // 4, at, :])

        def done(t, carry):
            lanes = pl.ds(pl.multiple_of(t * LANES, LANES), LANES)
            for rows, term in rows_of(t):
                o_ref[rows, lanes] = o_ref[rows, lanes] + term
            return carry

        def pending(t, carry):
            for rows, term in rows_of(t):
                l_t[t, rows, :] = l_t[t, rows, :] + term
            return carry

        lax.fori_loop(0, 12, done, 0, unroll=2)
        lax.fori_loop(12, 16, pending, 0, unroll=2)

    def sent(ch):
        for s in range(2):

            @pl.when(has_x[s])
            def _(s=s):
                x_copy(s, ch).wait_send()

            @pl.when(has_y[s])
            def _(s=s):
                y_copy(s, ch).wait_send()

    for s, r in corners:

        @pl.when(outer_one[s, r])
        def _(s=s, r=r):
            along_y(s, r, edge).start()

        @pl.when(cross_x[s, r])
        def _(s=s, r=r):
            along_x(s, r).start()

        @pl.when(inner_one[s, r])
        def _(s=s, r=r):
            across(s, r).start()

    send_x(0, 0)

    send_x(0, 3)

    send_y(0, 0)
    send_y(1, 0)

    send_x(1, 0)

    for s, r in corners:

        @pl.when(inner_one[s, r])
        def _(s=s, r=r):
            k = 2 * s + r
            along_x(1 - s, r).wait_recv()
            across(1 - s, 1 - r).wait_recv()
            passed[k] = edge_x[k] + edge_d[k] + edge[k]
            along_y(s, r, passed).start()

    send_y(0, 3)
    send_y(1, 3)

    send_x(1, 3)

    finish(1)

    finish(2)

    sent(1)

    sent(2)

    finish(0)

    sent(0)

    for s, r in corners:

        @pl.when(has_y[r])
        def _(s=s, r=r):
            along_y(s, 1 - r, edge).wait_recv()

        @pl.when(alone[s, r])
        def _(s=s, r=r):
            along_x(1 - s, r).wait_recv()

    for s, r in corners:

        @pl.when(has_y[r])
        def _(s=s, r=r):
            along_y(s, r, edge).wait_send()

        @pl.when(cross_x[s, r])
        def _(s=s, r=r):
            along_x(s, r).wait_send()

        @pl.when(inner_one[s, r])
        def _(s=s, r=r):
            across(s, r).wait_send()

    finish_edges()

    finish(3)

    sent(3)


def third_direction_kernel(x_ref, o_hbm, out, sem):
    tiles = out.shape[1] // LANES
    lane = lax.broadcasted_iota(jnp.int32, (8, LANES), 1)
    point = lane % 8
    shared = (point == 7) | (point == 0)
    swap = jnp.where(point == 7, (lane + 1) % LANES, jnp.where(point == 0, (lane + LANES - 1) % LANES, lane))
    head, tail = lane == 0, lane == LANES - 1
    first, last = shared & (lane > 0), shared & (lane < LANES - 1)

    def copy(i):
        rows = pl.ds(8 * i, 8)
        return pltpu.make_async_copy(out.at[rows], o_hbm.at[rows], sem.at[i])

    count = out.shape[0] // 8
    for i in range(count):
        rows = slice(8 * i, 8 * i + 8)
        own = [x_ref[rows, LANES * t:LANES * (t + 1)] for t in range(tiles)]
        other = [jnp.take_along_axis(v, swap, axis=1) for v in own]
        for t in range(tiles):
            take = other[t]
            if t > 0:
                take = jnp.where(head, other[t - 1], take)
            if t < tiles - 1:
                take = jnp.where(tail, other[t + 1], take)
            mask = first if t == 0 else last if t == tiles - 1 else shared
            out[rows, LANES * t:LANES * (t + 1)] = own[t] + jnp.where(mask, take, 0.0)
        copy(i).start()
    for i in range(count):
        copy(i).wait()


def solution(mesh):
    sizes = (mesh.shape["gx"], mesh.shape["gy"], mesh.shape["gz"])

    def local(values, geometry):
        tables = jnp.asarray(np.stack([lane_table(DERIVATIVE.T), lane_table(DERIVATIVE)]))
        rows, length = 192, values.shape[3]
        vmem = pl.BlockSpec(memory_space=pltpu.VMEM)
        hbm = pl.BlockSpec(memory_space=pltpu.HBM)
        dma = pltpu.SemaphoreType.DMA
        summed = pl.pallas_call(
            functools.partial(exchange_kernel, sizes),
            name="exchange",
            out_shape=pltpu.VMEM((rows, length), F32),
            in_specs=[hbm, hbm, hbm],
            out_specs=vmem,
            scratch_shapes=[
                pltpu.VMEM(geometry.shape, F32),
                pltpu.VMEM((16, rows, LANES), F32),
                pltpu.VMEM((16, rows, LANES), F32),
                pltpu.VMEM((2, 256, 256), BF16),
                pltpu.VMEM((16, 48, LANES), F32),
            ]
            + [pltpu.VMEM((2, rows, LANES), F32)] * 5
            + [pltpu.VMEM((2, 4, 104, LANES), F32)] * 4
            + [pltpu.VMEM((2, rows, LANES), F32)]
            + [pltpu.VMEM((4, 48, LANES), F32)] * 5
            + [dma(()), dma((16,)), dma(())]
            + [dma((2, 4))] * 4
            + [dma((2,))] * 2
            + [dma((4,))] * 6,
            compiler_params=pltpu.CompilerParams(collective_id=0, has_side_effects=True, vmem_limit_bytes=16 << 20),
        )(
            pltpu.with_memory_space_constraint(values.reshape(rows, length), pltpu.HBM),
            pltpu.with_memory_space_constraint(geometry, pltpu.HBM),
            pltpu.with_memory_space_constraint(tables, pltpu.HBM),
        )
        out = pl.pallas_call(
            third_direction_kernel,
            name="third",
            out_shape=jax.ShapeDtypeStruct((rows, length), F32),
            in_specs=[vmem],
            out_specs=hbm,
            scratch_shapes=[pltpu.VMEM((rows, length), F32), dma((rows // 8,))],
            compiler_params=pltpu.CompilerParams(vmem_limit_bytes=8 << 20),
        )(summed)
        return out.reshape(values.shape)

    return jax.shard_map(
        local,
        mesh=mesh,
        in_specs=(P(None, "gx", "gy", "gz"), P(None, "gx", "gy", "gz")),
        out_specs=P(None, "gx", "gy", "gz"),
        check_vma=False,
    )
```

```python
import functools

import jax
import jax.numpy as jnp
import numpy as np
from jax import lax
from jax.experimental import pallas as pl
from jax.experimental.pallas import tpu as pltpu
from jax.sharding import PartitionSpec as P

MESH = pl.DeviceIdType.MESH
F32 = jnp.float32
BF16 = jnp.bfloat16
LANES = 128

interior_points = [
    -0.8717401485096066,
    -0.5917001814331423,
    -0.2092992179024789,
    0.2092992179024789,
    0.5917001814331423,
    0.8717401485096066,
]


def legendre_seven(point):
    previous = 1.0
    current = point
    for order in range(1, 7):
        following = ((2 * order + 1) * point * current - order * previous) / (order + 1)
        previous = current
        current = following
    return current


def gll_tables():
    degree = 7
    points = [-1.0] + interior_points + [1.0]
    values = [legendre_seven(point) for point in points]
    node_count = degree + 1
    weights = np.array([2.0 / (degree * (degree + 1) * value * value) for value in values])
    derivative = np.zeros((node_count, node_count))
    for row_index in range(node_count):
        for col_index in range(node_count):
            if row_index != col_index:
                derivative[row_index, col_index] = values[row_index] / (
                    values[col_index] * (points[row_index] - points[col_index])
                )
    derivative[0, 0] = -degree * (degree + 1) / 4.0
    derivative[node_count - 1, node_count - 1] = degree * (degree + 1) / 4.0
    return derivative, weights


DERIVATIVE, WEIGHTS = gll_tables()
WEIGHTS = [float(w) for w in WEIGHTS]


def halves(matrix):
    plus = [[float(0.5 * (matrix[a, b] - matrix[a, 7 - b])) for b in range(4)] for a in range(4)]
    minus = [[float(0.5 * (matrix[a, b] + matrix[a, 7 - b])) for b in range(4)] for a in range(4)]
    return plus, minus


GRAD = halves(DERIVATIVE)
BACK = halves(DERIVATIVE.T)
BACK_X = halves(DERIVATIVE.T * np.array(WEIGHTS)[None, :])


def apply_halves(tables, planes):
    plus, minus = tables
    diff = [planes[b] - planes[7 - b] for b in range(4)]
    total = [planes[b] + planes[7 - b] for b in range(4)]
    out = [None] * 8
    for a in range(4):
        p = plus[a][0] * diff[0]
        q = minus[a][0] * total[0]
        for b in range(1, 4):
            p = p + plus[a][b] * diff[b]
            q = q + minus[a][b] * total[b]
        out[a] = p + q
        out[7 - a] = p - q
    return out


def lane_table(matrix):
    full = np.kron(np.eye(16), matrix).astype(np.float32)
    high = full.astype(BF16).astype(np.float32)
    row = np.concatenate([high, full - high], axis=1)
    return np.concatenate([row, row], axis=0).astype(BF16)


def lane_apply(rows, table):
    high = rows.astype(BF16)
    low = (rows - high.astype(F32)).astype(BF16)
    both = jnp.dot(jnp.concatenate([high, low], axis=1), table, preferred_element_type=F32)
    return both[:, :LANES] + both[:, LANES:]


def weight_vector(index):
    out = jnp.full(index.shape, WEIGHTS[0], F32)
    for i in range(1, 8):
        out = jnp.where(index % 8 == i, WEIGHTS[i], out)
    return out


def exchange_kernel(
    sizes,
    u_hbm, g_hbm, tables_hbm, o_ref,
    g_ref, u_t, l_t, tab, geo, s_gy, s_gz, s_fy, s_fz, s_ox,
    xf, yf, rx, ry, zr, edge, edge_y, edge_x, edge_d, passed,
    g_sem, in_sem, tab_sem, xs, xr, ys, yr, zs, zrs, eys, eyr, exs, exr, eds, edr,
):
    nx, ny, nz = sizes
    ix, iy, iz = lax.axis_index("gx"), lax.axis_index("gy"), lax.axis_index("gz")
    parity = iy % 2
    has_x = [ix > 0, ix < nx - 1]
    has_y = [iy > 0, iy < ny - 1]
    has_z = [iz > 0, iz < nz - 1]
    no_x = [ix == 0, ix == nx - 1]
    no_y = [iy == 0, iy == ny - 1]
    step_of = [-1, 1]

    def load(t):
        return pltpu.make_async_copy(
            u_hbm.at[:, pl.ds(pl.multiple_of(t * LANES, LANES), LANES)], u_t.at[t], in_sem.at[t]
        )

    barrier = pltpu.get_barrier_semaphore()
    dxm = 2 * parity - 1
    mid_x = [(parity == s) & has_x[s] for s in range(2)]
    greet = []
    for s in range(2):
        greet.append((has_x[s], {"gx": ix + step_of[s]}))
        greet.append((has_y[s], {"gy": iy + step_of[s]}))
        greet.append((has_z[s], {"gz": iz + step_of[s]}))
        for r in range(2):
            greet.append((mid_x[s] & has_y[r], {"gx": ix + step_of[s], "gy": iy + step_of[r]}))
    for there, device in greet:

        @pl.when(there)
        def _(device=device):
            pl.semaphore_signal(barrier, inc=1, device_id=device, device_id_type=MESH)

    tile_order = [4, 5, 6, 7, 0, 15, 8, 9, 10, 11, 1, 2, 3, 12, 13, 14]
    table_copy = pltpu.make_async_copy(tables_hbm, tab, tab_sem)
    geometry_copy = pltpu.make_async_copy(g_hbm, g_ref, g_sem)
    geometry_copy.start()
    load(tile_order[0]).start()
    table_copy.start()
    for t in tile_order[1:]:
        load(t).start()

    sub = lax.broadcasted_iota(jnp.int32, (8, LANES), 0)
    lane = lax.broadcasted_iota(jnp.int32, (8, LANES), 1)
    plane_weight = weight_vector(sub) * weight_vector(lane)
    geometry_copy.wait()
    for half in range(2):
        for k in range(6):
            row = jnp.broadcast_to(g_ref[k, 0, :, half * LANES:(half + 1) * LANES], (8, LANES))
            for j in range(8):
                picked = jnp.take_along_axis(row, lane // 8 + 16 * j, axis=1)
                geo[half * 8 + j, 8 * k:8 * k + 8, :] = picked * plane_weight

    even, odd = parity == 0, parity == 1
    corners = [(s, r) for s in range(2) for r in range(2)]
    hub = [has_x[0] & has_y[r] & even for r in range(2)]
    use_y = {(s, r): has_y[r] if s == 0 else has_y[r] & no_x[s] for s, r in corners}
    use_x = {(s, r): has_x[s] & (no_y[r] | even) for s, r in corners}
    use_d = {(s, r): has_x[s] & has_y[r] & (even if s == 0 else odd) for s, r in corners}
    early_y = {(s, r): has_y[r] & (no_x[s] | odd) if s == 0 else use_y[s, r] for s, r in corners}
    early_x = {(s, r): has_x[s] & no_y[r] if s == 0 else use_x[s, r] for s, r in corners}

    for s in range(2):

        @pl.when(no_x[s])
        def _(s=s):
            rx[s] = jnp.zeros(rx.shape[1:], F32)

        @pl.when(no_y[s])
        def _(s=s):
            ry[s] = jnp.zeros(ry.shape[1:], F32)

    for s, r in corners:
        k = 2 * s + r
        for used, land in ((use_y, edge_y), (use_x, edge_x), (use_d, edge_d)):

            @pl.when(jnp.logical_not(used[s, r]))
            def _(k=k, land=land):
                land[k] = jnp.zeros(land.shape[1:], F32)

    def compute(pair):
        for p, t in enumerate(pair):
            s_gz[p] = lane_apply(u_t[t], tab[0])
        for p, t in enumerate(pair):
            for c in range(3):
                uy = [u_t[t, pl.ds(64 * c + y, 8, stride=8), :] for y in range(8)]
                gy = apply_halves(GRAD, uy)
                for y in range(8):
                    s_gy[p, pl.ds(64 * c + y, 8, stride=8), :] = gy[y]
        for p, t in enumerate(pair):
            g00, g11, g22, g01, g02, g12 = [geo[t, 8 * k:8 * k + 8, :] for k in range(6)]
            for c in range(3):
                base = 64 * c
                ux = [u_t[t, base + 8 * x:base + 8 * x + 8, :] for x in range(8)]
                gx = apply_halves(GRAD, ux)
                fx = []
                for x in range(8):
                    rows = slice(base + 8 * x, base + 8 * x + 8)
                    a, b, d = gx[x], s_gy[p, rows, :], s_gz[p, rows, :]
                    fx.append(g00 * a + g01 * b + g02 * d)
                    s_fy[p, rows, :] = g01 * a + g11 * b + g12 * d
                    s_fz[p, rows, :] = g02 * a + g12 * b + g22 * d
                ox = apply_halves(BACK_X, fx)
                for x in range(8):
                    s_ox[p, base + 8 * x:base + 8 * x + 8, :] = ox[x]
            s_gz[p] = lane_apply(s_fz[p], tab[1])
        for p, t in enumerate(pair):
            for c in range(3):
                fy = [s_fy[p, pl.ds(64 * c + y, 8, stride=8), :] for y in range(8)]
                oy = apply_halves(BACK, fy)
                for y in range(8):
                    s_gy[p, pl.ds(64 * c + y, 8, stride=8), :] = oy[y]
        for p, t in enumerate(pair):
            for c in range(3):
                for x in range(8):
                    rows = slice(64 * c + 8 * x, 64 * c + 8 * x + 8)
                    l_t[t, rows, :] = s_ox[p, rows, :] + WEIGHTS[x] * (s_gy[p, rows, :] + s_gz[p, rows, :])

    def faces(t):
        ch, tt = t // 4, t % 4
        for c in range(3):
            at = pl.ds(4 + 4 * c + tt, 8, stride=12)
            for s in range(2):
                first = 64 * c + 56 * s
                xf[s, ch, at, :] = l_t[t, first:first + 8, :]
                yf[s, ch, at, :] = l_t[t, pl.ds(64 * c + 7 * s, 8, stride=8), :]

    body = pl.ds(16, 72)

    def face_copy(buf, land, send, recv, axis, index, s, ch):
        return pltpu.make_async_remote_copy(
            src_ref=buf.at[s, ch, body], dst_ref=land.at[1 - s, ch, body],
            send_sem=send.at[s, ch], recv_sem=recv.at[1 - s, ch],
            device_id={axis: index + step_of[s]}, device_id_type=MESH,
        )

    def x_copy(s, ch):
        return face_copy(xf, rx, xs, xr, "gx", ix, s, ch)

    def y_copy(s, ch):
        return face_copy(yf, ry, ys, yr, "gy", iy, s, ch)

    def send_x(s, ch):
        @pl.when(has_x[s])
        def _():
            x_copy(s, ch).start()

    def send_y(s, ch):
        @pl.when(has_y[s])
        def _():
            y_copy(s, ch).start()

    def z_copy(s):
        return pltpu.make_async_remote_copy(
            src_ref=l_t.at[15 * s], dst_ref=zr.at[1 - s], send_sem=zs.at[s], recv_sem=zrs.at[1 - s],
            device_id={"gz": iz + step_of[s]}, device_id_type=MESH,
        )

    table_copy.wait()

    def step(i, carry):
        first = jnp.where(i < 2, 2 * i + 4, jnp.where(i == 2, 0, jnp.where(i < 5, 2 * i + 2, jnp.where(i < 7, 2 * i - 9, 13))))
        second = jnp.where(i == 2, 15, jnp.where(i == 6, 12, first + 1))
        for t in (first, second):
            load(t).wait()
        compute((first, second))
        for t in (first, second):
            faces(t)

        @pl.when(i == 1)
        def _():
            pl.semaphore_wait(barrier, sum(there.astype(jnp.int32) for there, _ in greet))
            send_x(0, 1)
            send_y(0, 1)
            send_y(1, 1)
            send_x(1, 1)

        @pl.when(i == 4)
        def _():
            send_x(0, 2)
            send_y(0, 2)
            send_y(1, 2)
            send_x(1, 2)

        @pl.when(i == 2)
        def _():
            for s in range(2):

                @pl.when(has_z[s])
                def _(s=s):
                    z_copy(s).start()

        return carry

    lax.fori_loop(0, 8, step, 0)

    wide = lax.broadcasted_iota(jnp.int32, (192, LANES), 1)
    for s in range(2):

        @pl.when(has_z[s])
        def _(s=s):
            z_copy(s).wait_send()
            z_copy(1 - s).wait_recv()
            landed = pltpu.roll(zr[s], 1 if s == 0 else LANES - 1, 1)
            l_t[15 * s] = l_t[15 * s] + jnp.where(wide == (LANES - 1) * s, landed, 0.0)
            faces(15 * s)

    for s, r in corners:
        for ch in range(4):
            first = 4 + 84 * r
            edge[2 * s + r, 12 * ch:12 * ch + 12, :] = xf[s, ch, first:first + 12, :]

    def edge_copy(s, r, src, land, send, recv, dx, dy):
        k = 2 * s + r
        there = 2 * (1 - s if dx else s) + (1 - r if dy else r)
        device = {}
        if dx:
            device["gx"] = ix + step_of[s]
        if dy:
            device["gy"] = iy + step_of[r]
        return pltpu.make_async_remote_copy(
            src_ref=src, dst_ref=land.at[there], send_sem=send.at[k], recv_sem=recv.at[there],
            device_id=device, device_id_type=MESH,
        )

    def along_y(s, r, src=None):
        return edge_copy(s, r, edge.at[2 * s + r] if src is None else src, edge_y, eys, eyr, False, True)

    def along_x(s, r, src=None):
        return edge_copy(s, r, edge.at[2 * s + r] if src is None else src, edge_x, exs, exr, True, False)

    def across(s, r, src=None):
        return edge_copy(s, r, edge.at[2 * s + r] if src is None else src, edge_d, eds, edr, True, True)

    transverse = lax.broadcasted_iota(jnp.int32, (8, LANES), 0)
    inner = (transverse > 0) & (transverse < 7)

    def finish(ch):
        for s in range(2):

            @pl.when(has_x[s])
            def _(s=s):
                x_copy(1 - s, ch).wait_recv()

            @pl.when(has_y[s])
            def _(s=s):
                y_copy(1 - s, ch).wait_recv()

        def tile(tt, carry):
            t = 4 * ch + tt
            lanes = pl.ds(pl.multiple_of(t * LANES, LANES), LANES)
            for c in range(3):
                at = pl.ds(4 + 4 * c + tt, 8, stride=12)
                for s in range(2):
                    rows = slice(64 * c + 56 * s, 64 * c + 56 * s + 8)
                    l_t[t, rows, :] = l_t[t, rows, :] + jnp.where(inner, rx[s, ch, at, :], 0.0)
                for s in range(2):
                    rows = pl.ds(64 * c + 7 * s, 8, stride=8)
                    l_t[t, rows, :] = l_t[t, rows, :] + jnp.where(inner, ry[s, ch, at, :], 0.0)
            o_ref[:, lanes] = l_t[t]
            return carry

        lax.fori_loop(0, 4, tile, 0)

    def finish_edges():
        for s, r in corners:
            k, first = 2 * s + r, 4 + 84 * r
            for ch in range(4):
                part = slice(12 * ch, 12 * ch + 12)
                xf[s, ch, first:first + 12, :] = edge_y[k, part, :] + edge_x[k, part, :] + edge_d[k, part, :]

        def rows_of(t):
            for c in range(3):
                at = pl.ds(4 + 4 * c + t % 4, 8, stride=12)
                for s in range(2):
                    rows = slice(64 * c + 56 * s, 64 * c + 56 * s + 8)
                    yield rows, jnp.where(inner, 0.0, xf[s, t // 4, at, :])

        def done(t, carry):
            lanes = pl.ds(pl.multiple_of(t * LANES, LANES), LANES)
            for rows, term in rows_of(t):
                o_ref[rows, lanes] = o_ref[rows, lanes] + term
            return carry

        def pending(t, carry):
            for rows, term in rows_of(t):
                l_t[t, rows, :] = l_t[t, rows, :] + term
            return carry

        lax.fori_loop(0, 12, done, 0, unroll=2)
        lax.fori_loop(12, 16, pending, 0, unroll=2)

    def sent(ch):
        for s in range(2):

            @pl.when(has_x[s])
            def _(s=s):
                x_copy(s, ch).wait_send()

            @pl.when(has_y[s])
            def _(s=s):
                y_copy(s, ch).wait_send()

    for s, r in corners:

        @pl.when(early_y[s, r])
        def _(s=s, r=r):
            along_y(s, r).start()

        @pl.when(early_x[s, r])
        def _(s=s, r=r):
            along_x(s, r).start()

        if s == 1:

            @pl.when(use_d[s, r])
            def _(s=s, r=r):
                across(s, r).start()

    send_x(0, 0)

    send_y(0, 0)
    send_y(1, 0)

    send_x(1, 0)

    for r in (1, 0):

        @pl.when(hub[r])
        def _(r=r):
            along_y(0, 1 - r).wait_recv()
            across(1, 1 - r).wait_recv()
            along_x(1, r).wait_recv()
            passed[3 * r] = edge[r] + edge_d[r] + edge_y[r]
            passed[3 * r + 1] = edge[r] + edge_x[r] + edge_y[r]
            passed[3 * r + 2] = edge[r] + edge_x[r] + edge_d[r]
            across(0, r, passed.at[3 * r + 1]).start()
            along_x(0, r, passed.at[3 * r]).start()
            along_y(0, r, passed.at[3 * r + 2]).start()

    send_x(0, 3)

    send_y(0, 3)
    send_y(1, 3)

    send_x(1, 3)

    finish(1)

    finish(2)

    sent(1)

    sent(2)

    finish(0)

    sent(0)

    for s, r in corners:

        @pl.when(early_y[s, r])
        def _(s=s, r=r):
            along_y(s, 1 - r).wait_recv()

        @pl.when(early_x[s, r])
        def _(s=s, r=r):
            along_x(1 - s, r).wait_recv()

        if s == 1:

            @pl.when(use_d[s, r])
            def _(s=s, r=r):
                across(1 - s, 1 - r).wait_recv()

    for s, r in corners:

        @pl.when(use_y[s, r])
        def _(s=s, r=r):
            along_y(s, r).wait_send()

        @pl.when(use_x[s, r])
        def _(s=s, r=r):
            along_x(s, r).wait_send()

        @pl.when(use_d[s, r])
        def _(s=s, r=r):
            across(s, r).wait_send()

    finish_edges()

    finish(3)

    sent(3)


def third_direction_kernel(x_ref, o_hbm, out, sem):
    tiles = out.shape[1] // LANES
    lane = lax.broadcasted_iota(jnp.int32, (8, LANES), 1)
    point = lane % 8
    shared = (point == 7) | (point == 0)
    swap = jnp.where(point == 7, (lane + 1) % LANES, jnp.where(point == 0, (lane + LANES - 1) % LANES, lane))
    head, tail = lane == 0, lane == LANES - 1
    first, last = shared & (lane > 0), shared & (lane < LANES - 1)

    def copy(i):
        rows = pl.ds(8 * i, 8)
        return pltpu.make_async_copy(out.at[rows], o_hbm.at[rows], sem.at[i])

    count = out.shape[0] // 8
    for i in range(count):
        rows = slice(8 * i, 8 * i + 8)
        own = [x_ref[rows, LANES * t:LANES * (t + 1)] for t in range(tiles)]
        other = [jnp.take_along_axis(v, swap, axis=1) for v in own]
        for t in range(tiles):
            take = other[t]
            if t > 0:
                take = jnp.where(head, other[t - 1], take)
            if t < tiles - 1:
                take = jnp.where(tail, other[t + 1], take)
            mask = first if t == 0 else last if t == tiles - 1 else shared
            out[rows, LANES * t:LANES * (t + 1)] = own[t] + jnp.where(mask, take, 0.0)
        copy(i).start()
    for i in range(count):
        copy(i).wait()


def solution(mesh):
    sizes = (mesh.shape["gx"], mesh.shape["gy"], mesh.shape["gz"])

    def local(values, geometry):
        tables = jnp.asarray(np.stack([lane_table(DERIVATIVE.T), lane_table(DERIVATIVE)]))
        rows, length = 192, values.shape[3]
        vmem = pl.BlockSpec(memory_space=pltpu.VMEM)
        hbm = pl.BlockSpec(memory_space=pltpu.HBM)
        dma = pltpu.SemaphoreType.DMA
        summed = pl.pallas_call(
            functools.partial(exchange_kernel, sizes),
            name="exchange",
            out_shape=pltpu.VMEM((rows, length), F32),
            in_specs=[hbm, hbm, hbm],
            out_specs=vmem,
            scratch_shapes=[
                pltpu.VMEM(geometry.shape, F32),
                pltpu.VMEM((16, rows, LANES), F32),
                pltpu.VMEM((16, rows, LANES), F32),
                pltpu.VMEM((2, 256, 256), BF16),
                pltpu.VMEM((16, 48, LANES), F32),
            ]
            + [pltpu.VMEM((2, rows, LANES), F32)] * 5
            + [pltpu.VMEM((2, 4, 104, LANES), F32)] * 4
            + [pltpu.VMEM((2, rows, LANES), F32)]
            + [pltpu.VMEM((4, 48, LANES), F32)] * 4
            + [pltpu.VMEM((6, 48, LANES), F32)]
            + [dma(()), dma((16,)), dma(())]
            + [dma((2, 4))] * 4
            + [dma((2,))] * 2
            + [dma((4,))] * 6,
            compiler_params=pltpu.CompilerParams(collective_id=0, has_side_effects=True, vmem_limit_bytes=16 << 20),
        )(
            pltpu.with_memory_space_constraint(values.reshape(rows, length), pltpu.HBM),
            pltpu.with_memory_space_constraint(geometry, pltpu.HBM),
            pltpu.with_memory_space_constraint(tables, pltpu.HBM),
        )
        out = pl.pallas_call(
            third_direction_kernel,
            name="third",
            out_shape=jax.ShapeDtypeStruct((rows, length), F32),
            in_specs=[vmem],
            out_specs=hbm,
            scratch_shapes=[pltpu.VMEM((rows, length), F32), dma((rows // 8,))],
            compiler_params=pltpu.CompilerParams(vmem_limit_bytes=8 << 20),
        )(summed)
        return out.reshape(values.shape)

    return jax.shard_map(
        local,
        mesh=mesh,
        in_specs=(P(None, "gx", "gy", "gz"), P(None, "gx", "gy", "gz")),
        out_specs=P(None, "gx", "gy", "gz"),
        check_vma=False,
    )
```

```python
import functools

import jax
import jax.numpy as jnp
import numpy as np
from jax import lax
from jax.experimental import pallas as pl
from jax.experimental.pallas import tpu as pltpu
from jax.sharding import PartitionSpec as P

MESH = pl.DeviceIdType.MESH
F32 = jnp.float32
BF16 = jnp.bfloat16
LANES = 128

interior_points = [
    -0.8717401485096066,
    -0.5917001814331423,
    -0.2092992179024789,
    0.2092992179024789,
    0.5917001814331423,
    0.8717401485096066,
]


def legendre_seven(point):
    previous = 1.0
    current = point
    for order in range(1, 7):
        following = ((2 * order + 1) * point * current - order * previous) / (order + 1)
        previous = current
        current = following
    return current


def gll_tables():
    degree = 7
    points = [-1.0] + interior_points + [1.0]
    values = [legendre_seven(point) for point in points]
    node_count = degree + 1
    weights = np.array([2.0 / (degree * (degree + 1) * value * value) for value in values])
    derivative = np.zeros((node_count, node_count))
    for row_index in range(node_count):
        for col_index in range(node_count):
            if row_index != col_index:
                derivative[row_index, col_index] = values[row_index] / (
                    values[col_index] * (points[row_index] - points[col_index])
                )
    derivative[0, 0] = -degree * (degree + 1) / 4.0
    derivative[node_count - 1, node_count - 1] = degree * (degree + 1) / 4.0
    return derivative, weights


DERIVATIVE, WEIGHTS = gll_tables()
WEIGHTS = [float(w) for w in WEIGHTS]


def halves(matrix):
    plus = [[float(0.5 * (matrix[a, b] - matrix[a, 7 - b])) for b in range(4)] for a in range(4)]
    minus = [[float(0.5 * (matrix[a, b] + matrix[a, 7 - b])) for b in range(4)] for a in range(4)]
    return plus, minus


GRAD = halves(DERIVATIVE)
BACK = halves(DERIVATIVE.T)
BACK_X = halves(DERIVATIVE.T * np.array(WEIGHTS)[None, :])


def apply_halves(tables, planes):
    plus, minus = tables
    diff = [planes[b] - planes[7 - b] for b in range(4)]
    total = [planes[b] + planes[7 - b] for b in range(4)]
    out = [None] * 8
    for a in range(4):
        p = plus[a][0] * diff[0]
        q = minus[a][0] * total[0]
        for b in range(1, 4):
            p = p + plus[a][b] * diff[b]
            q = q + minus[a][b] * total[b]
        out[a] = p + q
        out[7 - a] = p - q
    return out


def lane_table(matrix):
    full = np.kron(np.eye(16), matrix).astype(np.float32)
    high = full.astype(BF16).astype(np.float32)
    row = np.concatenate([high, full - high], axis=1)
    return np.concatenate([row, row], axis=0).astype(BF16)


def lane_apply(rows, table):
    high = rows.astype(BF16)
    low = (rows - high.astype(F32)).astype(BF16)
    both = jnp.dot(jnp.concatenate([high, low], axis=1), table, preferred_element_type=F32)
    return both[:, :LANES] + both[:, LANES:]


def weight_vector(index):
    out = jnp.full(index.shape, WEIGHTS[0], F32)
    for i in range(1, 8):
        out = jnp.where(index % 8 == i, WEIGHTS[i], out)
    return out


def exchange_kernel(
    sizes,
    u_hbm, g_hbm, tables_hbm, o_ref,
    g_ref, u_t, l_t, tab, geo, s_gy, s_gz, s_fy, s_fz, s_ox,
    xf, yf, rx, ry, zr, edge, edge_y, edge_x, edge_d, passed,
    g_sem, in_sem, tab_sem, xs, xr, ys, yr, zs, zrs, eys, eyr, exs, exr, eds, edr,
):
    nx, ny, nz = sizes
    ix, iy, iz = lax.axis_index("gx"), lax.axis_index("gy"), lax.axis_index("gz")
    parity = iy % 2
    has_x = [ix > 0, ix < nx - 1]
    has_y = [iy > 0, iy < ny - 1]
    has_z = [iz > 0, iz < nz - 1]
    no_x = [ix == 0, ix == nx - 1]
    no_y = [iy == 0, iy == ny - 1]
    step_of = [-1, 1]

    def load(t):
        return pltpu.make_async_copy(
            u_hbm.at[:, pl.ds(pl.multiple_of(t * LANES, LANES), LANES)], u_t.at[t], in_sem.at[t]
        )

    barrier = pltpu.get_barrier_semaphore()
    dxm = 2 * parity - 1
    mid_x = [(parity == s) & has_x[s] for s in range(2)]
    greet = []
    for s in range(2):
        greet.append((has_x[s], {"gx": ix + step_of[s]}))
        greet.append((has_y[s], {"gy": iy + step_of[s]}))
        greet.append((has_z[s], {"gz": iz + step_of[s]}))
        for r in range(2):
            greet.append((mid_x[s] & has_y[r], {"gx": ix + step_of[s], "gy": iy + step_of[r]}))
    for there, device in greet:

        @pl.when(there)
        def _(device=device):
            pl.semaphore_signal(barrier, inc=1, device_id=device, device_id_type=MESH)

    tile_order = [4, 5, 6, 7, 0, 15, 8, 9, 10, 11, 1, 2, 3, 12, 13, 14]
    table_copy = pltpu.make_async_copy(tables_hbm, tab, tab_sem)
    geometry_copy = pltpu.make_async_copy(g_hbm, g_ref, g_sem)
    geometry_copy.start()
    load(tile_order[0]).start()
    table_copy.start()
    for t in tile_order[1:]:
        load(t).start()

    sub = lax.broadcasted_iota(jnp.int32, (8, LANES), 0)
    lane = lax.broadcasted_iota(jnp.int32, (8, LANES), 1)
    plane_weight = weight_vector(sub) * weight_vector(lane)
    geometry_copy.wait()
    for half in range(2):
        for k in range(6):
            row = jnp.broadcast_to(g_ref[k, 0, :, half * LANES:(half + 1) * LANES], (8, LANES))
            for j in range(8):
                picked = jnp.take_along_axis(row, lane // 8 + 16 * j, axis=1)
                geo[half * 8 + j, 8 * k:8 * k + 8, :] = picked * plane_weight

    even, odd = parity == 0, parity == 1
    corners = [(s, r) for s in range(2) for r in range(2)]
    hub = [has_x[0] & has_y[r] & even for r in range(2)]
    use_y = {(s, r): has_y[r] if s == 0 else has_y[r] & no_x[s] for s, r in corners}
    use_x = {(s, r): has_x[s] & (no_y[r] | even) for s, r in corners}
    use_d = {(s, r): has_x[s] & has_y[r] & (even if s == 0 else odd) for s, r in corners}
    early_y = {(s, r): has_y[r] & (no_x[s] | odd) if s == 0 else use_y[s, r] for s, r in corners}
    early_x = {(s, r): has_x[s] & no_y[r] if s == 0 else use_x[s, r] for s, r in corners}

    for s in range(2):

        @pl.when(no_x[s])
        def _(s=s):
            rx[s] = jnp.zeros(rx.shape[1:], F32)

        @pl.when(no_y[s])
        def _(s=s):
            ry[s] = jnp.zeros(ry.shape[1:], F32)

    for s, r in corners:
        k = 2 * s + r
        for used, land in ((use_y, edge_y), (use_x, edge_x), (use_d, edge_d)):

            @pl.when(jnp.logical_not(used[s, r]))
            def _(k=k, land=land):
                land[k] = jnp.zeros(land.shape[1:], F32)

    def compute(pair):
        for p, t in enumerate(pair):
            s_gz[p] = lane_apply(u_t[t], tab[0])
        for p, t in enumerate(pair):
            for c in range(3):
                uy = [u_t[t, pl.ds(64 * c + y, 8, stride=8), :] for y in range(8)]
                gy = apply_halves(GRAD, uy)
                for y in range(8):
                    s_gy[p, pl.ds(64 * c + y, 8, stride=8), :] = gy[y]
        for p, t in enumerate(pair):
            g00, g11, g22, g01, g02, g12 = [geo[t, 8 * k:8 * k + 8, :] for k in range(6)]
            for c in range(3):
                base = 64 * c
                ux = [u_t[t, base + 8 * x:base + 8 * x + 8, :] for x in range(8)]
                gx = apply_halves(GRAD, ux)
                fx = []
                for x in range(8):
                    rows = slice(base + 8 * x, base + 8 * x + 8)
                    a, b, d = gx[x], s_gy[p, rows, :], s_gz[p, rows, :]
                    fx.append(g00 * a + g01 * b + g02 * d)
                    s_fy[p, rows, :] = g01 * a + g11 * b + g12 * d
                    s_fz[p, rows, :] = g02 * a + g12 * b + g22 * d
                ox = apply_halves(BACK_X, fx)
                for x in range(8):
                    s_ox[p, base + 8 * x:base + 8 * x + 8, :] = ox[x]
            s_gz[p] = lane_apply(s_fz[p], tab[1])
        for p, t in enumerate(pair):
            for c in range(3):
                fy = [s_fy[p, pl.ds(64 * c + y, 8, stride=8), :] for y in range(8)]
                oy = apply_halves(BACK, fy)
                for y in range(8):
                    s_gy[p, pl.ds(64 * c + y, 8, stride=8), :] = oy[y]
        for p, t in enumerate(pair):
            for c in range(3):
                for x in range(8):
                    rows = slice(64 * c + 8 * x, 64 * c + 8 * x + 8)
                    l_t[t, rows, :] = s_ox[p, rows, :] + WEIGHTS[x] * (s_gy[p, rows, :] + s_gz[p, rows, :])

    def faces(t):
        ch, tt = t // 4, t % 4
        for c in range(3):
            at = pl.ds(4 + 4 * c + tt, 8, stride=12)
            for s in range(2):
                first = 64 * c + 56 * s
                xf[s, ch, at, :] = l_t[t, first:first + 8, :]
                yf[s, ch, at, :] = l_t[t, pl.ds(64 * c + 7 * s, 8, stride=8), :]

    body = pl.ds(16, 72)

    def face_copy(buf, land, send, recv, axis, index, s, ch):
        return pltpu.make_async_remote_copy(
            src_ref=buf.at[s, ch, body], dst_ref=land.at[1 - s, ch, body],
            send_sem=send.at[s, ch], recv_sem=recv.at[1 - s, ch],
            device_id={axis: index + step_of[s]}, device_id_type=MESH,
        )

    def x_copy(s, ch):
        return face_copy(xf, rx, xs, xr, "gx", ix, s, ch)

    def y_copy(s, ch):
        return face_copy(yf, ry, ys, yr, "gy", iy, s, ch)

    def send_x(s, ch):
        @pl.when(has_x[s])
        def _():
            x_copy(s, ch).start()

    def send_y(s, ch):
        @pl.when(has_y[s])
        def _():
            y_copy(s, ch).start()

    def z_copy(s):
        return pltpu.make_async_remote_copy(
            src_ref=l_t.at[15 * s], dst_ref=zr.at[1 - s], send_sem=zs.at[s], recv_sem=zrs.at[1 - s],
            device_id={"gz": iz + step_of[s]}, device_id_type=MESH,
        )

    table_copy.wait()

    def step(i, carry):
        first = jnp.where(i < 2, 2 * i + 4, jnp.where(i == 2, 0, jnp.where(i < 5, 2 * i + 2, jnp.where(i < 7, 2 * i - 9, 13))))
        second = jnp.where(i == 2, 15, jnp.where(i == 6, 12, first + 1))
        for t in (first, second):
            load(t).wait()
        compute((first, second))
        for t in (first, second):
            faces(t)

        @pl.when(i == 1)
        def _():
            pl.semaphore_wait(barrier, sum(there.astype(jnp.int32) for there, _ in greet))
            send_x(0, 1)
            send_y(0, 1)
            send_y(1, 1)
            send_x(1, 1)

        @pl.when(i == 4)
        def _():
            send_x(0, 2)
            send_y(0, 2)
            send_y(1, 2)

        @pl.when(i == 2)
        def _():
            for s in range(2):

                @pl.when(has_z[s])
                def _(s=s):
                    z_copy(s).start()

        return carry

    lax.fori_loop(0, 8, step, 0)

    wide = lax.broadcasted_iota(jnp.int32, (192, LANES), 1)
    for s in range(2):

        @pl.when(has_z[s])
        def _(s=s):
            z_copy(s).wait_send()
            z_copy(1 - s).wait_recv()
            landed = pltpu.roll(zr[s], 1 if s == 0 else LANES - 1, 1)
            l_t[15 * s] = l_t[15 * s] + jnp.where(wide == (LANES - 1) * s, landed, 0.0)
            faces(15 * s)

    for s, r in corners:
        for ch in range(4):
            first = 4 + 84 * r
            edge[2 * s + r, 12 * ch:12 * ch + 12, :] = xf[s, ch, first:first + 12, :]

    def edge_copy(s, r, src, land, send, recv, dx, dy):
        k = 2 * s + r
        there = 2 * (1 - s if dx else s) + (1 - r if dy else r)
        device = {}
        if dx:
            device["gx"] = ix + step_of[s]
        if dy:
            device["gy"] = iy + step_of[r]
        return pltpu.make_async_remote_copy(
            src_ref=src, dst_ref=land.at[there], send_sem=send.at[k], recv_sem=recv.at[there],
            device_id=device, device_id_type=MESH,
        )

    def along_y(s, r, src=None):
        return edge_copy(s, r, edge.at[2 * s + r] if src is None else src, edge_y, eys, eyr, False, True)

    def along_x(s, r, src=None):
        return edge_copy(s, r, edge.at[2 * s + r] if src is None else src, edge_x, exs, exr, True, False)

    def across(s, r, src=None):
        return edge_copy(s, r, edge.at[2 * s + r] if src is None else src, edge_d, eds, edr, True, True)

    transverse = lax.broadcasted_iota(jnp.int32, (8, LANES), 0)
    inner = (transverse > 0) & (transverse < 7)

    def finish(ch):
        for s in range(2):

            @pl.when(has_x[s])
            def _(s=s):
                x_copy(1 - s, ch).wait_recv()

            @pl.when(has_y[s])
            def _(s=s):
                y_copy(1 - s, ch).wait_recv()

        def tile(tt, carry):
            t = 4 * ch + tt
            lanes = pl.ds(pl.multiple_of(t * LANES, LANES), LANES)
            for c in range(3):
                at = pl.ds(4 + 4 * c + tt, 8, stride=12)
                for s in range(2):
                    rows = slice(64 * c + 56 * s, 64 * c + 56 * s + 8)
                    l_t[t, rows, :] = l_t[t, rows, :] + jnp.where(inner, rx[s, ch, at, :], 0.0)
                for s in range(2):
                    rows = pl.ds(64 * c + 7 * s, 8, stride=8)
                    l_t[t, rows, :] = l_t[t, rows, :] + jnp.where(inner, ry[s, ch, at, :], 0.0)
            o_ref[:, lanes] = l_t[t]
            return carry

        lax.fori_loop(0, 4, tile, 0)

    def finish_edges():
        for s, r in corners:
            k, first = 2 * s + r, 4 + 84 * r
            for ch in range(4):
                part = slice(12 * ch, 12 * ch + 12)
                xf[s, ch, first:first + 12, :] = edge_y[k, part, :] + edge_x[k, part, :] + edge_d[k, part, :]

        def rows_of(t):
            for c in range(3):
                at = pl.ds(4 + 4 * c + t % 4, 8, stride=12)
                for s in range(2):
                    rows = slice(64 * c + 56 * s, 64 * c + 56 * s + 8)
                    yield rows, jnp.where(inner, 0.0, xf[s, t // 4, at, :])

        def done(t, carry):
            lanes = pl.ds(pl.multiple_of(t * LANES, LANES), LANES)
            for rows, term in rows_of(t):
                o_ref[rows, lanes] = o_ref[rows, lanes] + term
            return carry

        def pending(t, carry):
            for rows, term in rows_of(t):
                l_t[t, rows, :] = l_t[t, rows, :] + term
            return carry

        lax.fori_loop(0, 12, done, 0, unroll=2)
        lax.fori_loop(12, 16, pending, 0, unroll=2)

    def sent(ch):
        for s in range(2):

            @pl.when(has_x[s])
            def _(s=s):
                x_copy(s, ch).wait_send()

            @pl.when(has_y[s])
            def _(s=s):
                y_copy(s, ch).wait_send()

    for s, r in corners:

        @pl.when(early_y[s, r])
        def _(s=s, r=r):
            along_y(s, r).start()

        @pl.when(early_x[s, r])
        def _(s=s, r=r):
            along_x(s, r).start()

        if s == 1:

            @pl.when(use_d[s, r])
            def _(s=s, r=r):
                across(s, r).start()

    send_x(1, 2)

    send_x(0, 0)

    send_y(0, 0)
    send_y(1, 0)

    for r in (1, 0):

        @pl.when(hub[r])
        def _(r=r):
            along_y(0, 1 - r).wait_recv()
            across(1, 1 - r).wait_recv()
            along_x(1, r).wait_recv()
            passed[3 * r] = edge[r] + edge_d[r] + edge_y[r]
            passed[3 * r + 1] = edge[r] + edge_x[r] + edge_y[r]
            passed[3 * r + 2] = edge[r] + edge_x[r] + edge_d[r]
            across(0, r, passed.at[3 * r + 1]).start()
            along_x(0, r, passed.at[3 * r]).start()
            along_y(0, r, passed.at[3 * r + 2]).start()

    send_x(0, 3)

    send_x(1, 0)

    send_y(0, 3)
    send_y(1, 3)

    send_x(1, 3)

    finish(1)

    finish(2)

    sent(1)

    sent(2)

    finish(0)

    sent(0)

    for s, r in corners:

        @pl.when(early_y[s, r])
        def _(s=s, r=r):
            along_y(s, 1 - r).wait_recv()

        @pl.when(early_x[s, r])
        def _(s=s, r=r):
            along_x(1 - s, r).wait_recv()

        if s == 1:

            @pl.when(use_d[s, r])
            def _(s=s, r=r):
                across(1 - s, 1 - r).wait_recv()

    for s, r in corners:

        @pl.when(use_y[s, r])
        def _(s=s, r=r):
            along_y(s, r).wait_send()

        @pl.when(use_x[s, r])
        def _(s=s, r=r):
            along_x(s, r).wait_send()

        @pl.when(use_d[s, r])
        def _(s=s, r=r):
            across(s, r).wait_send()

    finish_edges()

    finish(3)

    sent(3)


def third_direction_kernel(x_ref, o_hbm, out, sem):
    tiles = out.shape[1] // LANES
    lane = lax.broadcasted_iota(jnp.int32, (8, LANES), 1)
    point = lane % 8
    shared = (point == 7) | (point == 0)
    swap = jnp.where(point == 7, (lane + 1) % LANES, jnp.where(point == 0, (lane + LANES - 1) % LANES, lane))
    head, tail = lane == 0, lane == LANES - 1
    first, last = shared & (lane > 0), shared & (lane < LANES - 1)

    def copy(i):
        rows = pl.ds(8 * i, 8)
        return pltpu.make_async_copy(out.at[rows], o_hbm.at[rows], sem.at[i])

    count = out.shape[0] // 8
    for i in range(count):
        rows = slice(8 * i, 8 * i + 8)
        own = [x_ref[rows, LANES * t:LANES * (t + 1)] for t in range(tiles)]
        other = [jnp.take_along_axis(v, swap, axis=1) for v in own]
        for t in range(tiles):
            take = other[t]
            if t > 0:
                take = jnp.where(head, other[t - 1], take)
            if t < tiles - 1:
                take = jnp.where(tail, other[t + 1], take)
            mask = first if t == 0 else last if t == tiles - 1 else shared
            out[rows, LANES * t:LANES * (t + 1)] = own[t] + jnp.where(mask, take, 0.0)
        copy(i).start()
    for i in range(count):
        copy(i).wait()


def solution(mesh):
    sizes = (mesh.shape["gx"], mesh.shape["gy"], mesh.shape["gz"])

    def local(values, geometry):
        tables = jnp.asarray(np.stack([lane_table(DERIVATIVE.T), lane_table(DERIVATIVE)]))
        rows, length = 192, values.shape[3]
        vmem = pl.BlockSpec(memory_space=pltpu.VMEM)
        hbm = pl.BlockSpec(memory_space=pltpu.HBM)
        dma = pltpu.SemaphoreType.DMA
        summed = pl.pallas_call(
            functools.partial(exchange_kernel, sizes),
            name="exchange",
            out_shape=pltpu.VMEM((rows, length), F32),
            in_specs=[hbm, hbm, hbm],
            out_specs=vmem,
            scratch_shapes=[
                pltpu.VMEM(geometry.shape, F32),
                pltpu.VMEM((16, rows, LANES), F32),
                pltpu.VMEM((16, rows, LANES), F32),
                pltpu.VMEM((2, 256, 256), BF16),
                pltpu.VMEM((16, 48, LANES), F32),
            ]
            + [pltpu.VMEM((2, rows, LANES), F32)] * 5
            + [pltpu.VMEM((2, 4, 104, LANES), F32)] * 4
            + [pltpu.VMEM((2, rows, LANES), F32)]
            + [pltpu.VMEM((4, 48, LANES), F32)] * 4
            + [pltpu.VMEM((6, 48, LANES), F32)]
            + [dma(()), dma((16,)), dma(())]
            + [dma((2, 4))] * 4
            + [dma((2,))] * 2
            + [dma((4,))] * 6,
            compiler_params=pltpu.CompilerParams(collective_id=0, has_side_effects=True, vmem_limit_bytes=16 << 20),
        )(
            pltpu.with_memory_space_constraint(values.reshape(rows, length), pltpu.HBM),
            pltpu.with_memory_space_constraint(geometry, pltpu.HBM),
            pltpu.with_memory_space_constraint(tables, pltpu.HBM),
        )
        out = pl.pallas_call(
            third_direction_kernel,
            name="third",
            out_shape=jax.ShapeDtypeStruct((rows, length), F32),
            in_specs=[vmem],
            out_specs=hbm,
            scratch_shapes=[pltpu.VMEM((rows, length), F32), dma((rows // 8,))],
            compiler_params=pltpu.CompilerParams(vmem_limit_bytes=8 << 20),
        )(summed)
        return out.reshape(values.shape)

    return jax.shard_map(
        local,
        mesh=mesh,
        in_specs=(P(None, "gx", "gy", "gz"), P(None, "gx", "gy", "gz")),
        out_specs=P(None, "gx", "gy", "gz"),
        check_vma=False,
    )
```
